32 devices in a mesh: dp: 4 (over z), tensor: 8 (over y, x, core).
Axes of the slice: x: 2, y: 2, z: 4, core: 2. Of those that a mesh axis runs over, the one named last changes fastest.
Arguments:
- hidden_slots: bfloat16 [16, 96, 8192], P('dp', None, 'tensor'), may hold values from -6 to 6
- lengths: int32 [4, 4], replicated, may hold values from 1 to 96, 192 in all within a row
- owners: int32 [4, 4], replicated, may hold values from 0 to 3, as said below
- norm_gain: float32 [8192], replicated, may hold values from 0.25 to 1.75
- w_query: bfloat16 [8192, 8192], P(None, 'tensor'), may hold values from -0.0625 to 0.0625
- query_bias: float32 [8192], P('tensor'), may hold values from -3 to 3
- w_keyvalue: bfloat16 [8192, 2048], P('tensor'), may hold values from -0.0625 to 0.0625
- keyvalue_bias: float32 [2048], replicated, may hold values from -3 to 3
- grad_attention: bfloat16 [768, 8192], P('dp', 'tensor'), may hold values from -6 to 6
Outputs:
- attention: bfloat16 [768, 8192], P('dp', 'tensor')
- input_grad: bfloat16 [768, 8192], P('dp', 'tensor')
The draws below stay inside these ranges and needn't reach their ends.
Inputs may be any that keep to these rules, and one draw needn't show every extreme that they name: `owners`: every owner appears exactly once in each row and exactly once in each column j, so each micro-batch takes one rollout from every owner and each owner holds exactly one rollout in each of its 4 slots. `lengths`: each row sums to 192, and its largest entry is 96.
All inputs are finite; a program needn't handle non-finite values.
Results may differ from the reference program's by a relative error of at most 0.013.
Values may be sent and summed in bfloat16 or wider, within the bound.
No kernel may reach another device: no remote copies, remote signals or barrier semaphores. Data moves between devices by JAX's collectives and lax.ppermute only.
A program may use at most 64 MiB of HBM per device.

```python
import math
import jax
import jax.numpy as jnp
import numpy as np
from jax import lax

D = 8192
HEADS = 64
KV_HEADS = 8
HEAD_DIM = 128
TOK_DEV = 192
RPM = 4
LMAX = 96
SLOTS = 16
TOKENS = 768
N_DP = 4


def draw_owners(key, part):
    first_key = jax.random.fold_in(key, 101)
    second_key = jax.random.fold_in(key, 202)
    third_key = jax.random.fold_in(key, 303)
    relabel = jax.random.permutation(first_key, N_DP)
    standing = jax.random.permutation(second_key, N_DP)
    shifts = jax.random.permutation(third_key, N_DP)[:RPM]
    owner_table = relabel[(standing[:, None] + shifts[None, :]) % N_DP]
    return owner_table.astype(jnp.int32)


def block_scale(key, dims, shards, least, top_value):
    def one(dim, parts):
        draws = jax.random.uniform(jax.random.fold_in(jax.random.fold_in(key, 6), dim), (parts,), jnp.float32, least / len(shards), top_value / len(shards))
        return jnp.repeat(jnp.exp(draws), dims[dim] // parts).reshape((-1,) + (1,) * (len(dims) - dim - 1))

    level = one(*shards[0])
    for cut in shards[1:]:
        level = level * one(*cut)
    return level


def length_profile(number_of, total, bound, skew):
    portions = [(1 << 20) // math.isqrt(rank ** skew) + 1 for rank in range(2, number_of + 1)]
    surplus, holding = total - bound - (number_of - 1), [1] * (number_of - 1)
    while surplus > 0:
        movable = [i for i in range(number_of - 1) if holding[i] < bound]
        whole, remaining = sum([portions[i] for i in movable]), surplus
        for i in movable:
            more = min(bound - holding[i], max(1, remaining * portions[i] // whole), surplus)
            holding[i] = holding[i] + more
            surplus = surplus - more
    return np.array([bound] + holding)


def uneven_parts(stream_key, number_of, total, bound, slope):
    if number_of == 2:
        one = jax.random.randint(stream_key, (), max(1, total - bound), min(bound, total - 1) + 1)
        return jnp.stack([one, total - one])
    sizes = jnp.asarray(length_profile(number_of, total, bound, slope), jnp.int32)
    twos = (number_of - 1) // 2
    source_of, taker = sizes[1:1 + 2 * twos:2], sizes[2:2 + 2 * twos:2]
    room = jnp.minimum(source_of - 1, bound - taker)
    moved = jax.random.randint(jax.random.fold_in(stream_key, 1), (twos,), 0, 1 << 20) % (room + 1)
    sizes = sizes.at[1:1 + 2 * twos:2].set(source_of - moved).at[2:2 + 2 * twos:2].set(taker + moved)
    return sizes[jax.random.permutation(jax.random.fold_in(stream_key, 2), number_of)]


def gaussian(stream_key, extent, spread, bound, split=(), kind=jnp.bfloat16):
    level = block_scale(stream_key, extent, split, -0.22, 0.18) if split else 1.0
    result = jax.random.normal(stream_key, extent, jnp.float32) * spread * level
    return jnp.minimum(jnp.maximum(result, -bound), bound).astype(kind)


def setup_inputs(seed: int = 0) -> dict:
    seeds = jax.random.split(jax.random.key(seed), 10)
    hidden_slots = gaussian(seeds[0], (SLOTS, LMAX, D), 1.0, 6.0, ((0, 4), (2, 8)))
    lengths = jax.vmap(lambda own: uneven_parts(own, RPM, TOK_DEV, LMAX, 2))(jax.random.split(seeds[1], N_DP)).reshape((N_DP, RPM)).astype(jnp.int32)
    owners = draw_owners(jax.random.fold_in(seeds[9], 71), 0)
    norm_gain = jnp.clip(1.0 + 0.15 * jax.random.normal(seeds[3], (D,), jnp.float32), 0.25, 1.75)
    w_query = gaussian(seeds[4], (D, HEADS * HEAD_DIM), D ** -0.5, 0.0625, ((1, 8),))
    query_bias = gaussian(seeds[5], (HEADS * HEAD_DIM,), 0.5, 3.0, ((0, 8),), jnp.float32)
    w_keyvalue = gaussian(seeds[6], (D, 2 * KV_HEADS * HEAD_DIM), D ** -0.5, 0.0625, ((0, 8),))
    keyvalue_bias = gaussian(seeds[7], (2 * KV_HEADS * HEAD_DIM,), 0.5, 3.0, (), jnp.float32)
    grad_attention = gaussian(seeds[8], (TOKENS, HEADS * HEAD_DIM), 1.0, 6.0, ((0, 4), (1, 8)))
    return {"hidden_slots": hidden_slots, "lengths": lengths, "owners": owners, "norm_gain": norm_gain, "w_query": w_query, "query_bias": query_bias, "w_keyvalue": w_keyvalue, "keyvalue_bias": keyvalue_bias, "grad_attention": grad_attention}


EPSILON = 1e-06
ROPE_BASE = 1000000.0

def packing(length_row, row_count):
    starts = jnp.cumsum(length_row) - length_row
    places = jnp.arange(row_count, dtype=jnp.int32)
    segment = lax.optimization_barrier(jnp.sum((places[:, None] >= starts[None, 1:]).astype(jnp.int32), axis=1))
    onehot = (segment[:, None] == jnp.arange(length_row.shape[0], dtype=jnp.int32)[None, :]).astype(jnp.int32)
    offset = places - lax.optimization_barrier(jnp.sum(onehot * starts[None, :], axis=1))
    return (segment, offset, onehot)

def tables(offset, head_width):
    halfway = head_width // 2
    frequency = ROPE_BASE ** (-2.0 * jnp.arange(halfway, dtype=jnp.float32) / head_width)
    angles = offset.astype(jnp.float32)[:, None] * frequency[None, :]
    angles = jnp.concatenate([angles, angles], axis=1)
    return (jnp.cos(angles)[:, None, :], jnp.sin(angles)[:, None, :])

def rotate(values, cosine, sine_table):
    halfway = values.shape[-1] // 2
    turned = jnp.concatenate([-values[..., halfway:], values[..., :halfway]], axis=-1)
    return values * cosine + turned * sine_table

def unrotate(gradient, cosine, sine_table):
    halfway = gradient.shape[-1] // 2
    scaled = gradient * sine_table
    turned = jnp.concatenate([scaled[..., halfway:], -scaled[..., :halfway]], axis=-1)
    return gradient * cosine + turned

def normalize(hidden, norm_gain):
    widened = hidden.astype(jnp.float32)
    inverse = lax.rsqrt(lax.optimization_barrier(jnp.mean(widened * widened, axis=1)) + EPSILON)
    normed = (widened * inverse[:, None] * norm_gain).astype(jnp.bfloat16)
    return (widened, inverse, normed)

def masked_softmax(scores, allowed):
    scores = jnp.where(allowed, scores, -1e+30)
    highest = lax.optimization_barrier(jnp.max(scores, axis=-1, keepdims=True))
    exponent = jnp.where(allowed, jnp.exp(scores - highest), 0.0)
    return exponent / lax.optimization_barrier(jnp.sum(exponent, axis=-1, keepdims=True))

def contract_last(operand, weights):
    return lax.dot_general(operand, weights, (((1,), (1,)), ((), ())), preferred_element_type=jnp.float32)

def reference(hidden_slots, lengths, owners, norm_gain, w_query, query_bias, w_keyvalue, keyvalue_bias, grad_attention):
    flat_rows = hidden_slots.reshape(N_DP * RPM * LMAX, D)
    group_size = HEADS // KV_HEADS
    kv_width = KV_HEADS * HEAD_DIM
    score_scale = HEAD_DIM ** (-0.5)

    def micro_batch(batch_index):
        length_row = lax.dynamic_index_in_dim(lengths, batch_index, 0, keepdims=False)
        owner_row = lax.dynamic_index_in_dim(owners, batch_index, 0, keepdims=False)
        segment, offset, onehot = packing(length_row, TOK_DEV)
        source = lax.optimization_barrier(jnp.sum(onehot * owner_row[None, :], axis=1))
        row_index = ((source * RPM + segment) * LMAX + offset).astype(jnp.int32)
        hidden = jnp.take(flat_rows, row_index, axis=0)
        upstream = lax.dynamic_slice_in_dim(grad_attention, (batch_index * TOK_DEV).astype(jnp.int32), TOK_DEV, 0)
        upstream_wide = upstream.reshape(TOK_DEV, HEADS, HEAD_DIM).astype(jnp.float32)
        widened, inverse, normed = normalize(hidden, norm_gain)
        query_full = jnp.dot(normed, w_query, preferred_element_type=jnp.float32) + query_bias
        keyvalue = jnp.dot(normed, w_keyvalue, preferred_element_type=jnp.float32) + keyvalue_bias
        cosine, sine_table = tables(offset, HEAD_DIM)
        query_rot = rotate(query_full.reshape(TOK_DEV, HEADS, HEAD_DIM), cosine, sine_table).astype(jnp.bfloat16)
        key_rot = rotate(keyvalue[:, :kv_width].reshape(TOK_DEV, KV_HEADS, HEAD_DIM), cosine, sine_table).astype(jnp.bfloat16)
        value_heads = keyvalue[:, kv_width:].reshape(TOK_DEV, KV_HEADS, HEAD_DIM).astype(jnp.bfloat16)
        key_wide = jnp.repeat(key_rot, group_size, axis=1).astype(jnp.float32)
        value_wide = jnp.repeat(value_heads, group_size, axis=1).astype(jnp.float32)
        query_wide = query_rot.astype(jnp.float32)
        places = jnp.arange(TOK_DEV, dtype=jnp.int32)
        allowed = (segment[:, None] == segment[None, :]) & (places[None, :] <= places[:, None])
        scores = jnp.einsum('qhd,khd->hqk', query_wide, key_wide) * score_scale
        attn_weights = masked_softmax(scores, allowed[None])
        low_weights = lax.optimization_barrier(attn_weights.astype(jnp.bfloat16)).astype(jnp.float32)
        attended = jnp.einsum('hqk,khd->qhd', low_weights, value_wide).astype(jnp.bfloat16)
        weight_grad = jnp.einsum('qhd,khd->hqk', upstream_wide, value_wide)
        value_part = jnp.einsum('hqk,qhd->khd', low_weights, upstream_wide)
        row_inner = lax.optimization_barrier(jnp.sum(attn_weights * weight_grad, axis=-1, keepdims=True))
        score_grad = lax.optimization_barrier((attn_weights * (weight_grad - row_inner) * score_scale).astype(jnp.bfloat16)).astype(jnp.float32)
        query_grad = unrotate(jnp.einsum('hqk,khd->qhd', score_grad, key_wide), cosine, sine_table).astype(jnp.bfloat16)
        key_part = jnp.einsum('hqk,qhd->khd', score_grad, query_wide)
        key_grad = unrotate(key_part.reshape(TOK_DEV, KV_HEADS, group_size, HEAD_DIM).sum(axis=2), cosine, sine_table).astype(jnp.bfloat16)
        value_grad = value_part.reshape(TOK_DEV, KV_HEADS, group_size, HEAD_DIM).sum(axis=2).astype(jnp.bfloat16)
        kv_grad = jnp.concatenate([key_grad.reshape(TOK_DEV, kv_width), value_grad.reshape(TOK_DEV, kv_width)], axis=1)
        normed_grad = contract_last(query_grad.reshape(TOK_DEV, HEADS * HEAD_DIM), w_query) + contract_last(kv_grad, w_keyvalue)
        scaled = norm_gain * normed_grad
        row_stat = lax.optimization_barrier(jnp.mean(scaled * widened, axis=1))
        input_grad = (inverse[:, None] * scaled - widened * (inverse ** 3 * row_stat)[:, None]).astype(jnp.bfloat16)
        return (attended.reshape(TOK_DEV, HEADS * HEAD_DIM), input_grad)
    results = lax.map(micro_batch, jnp.arange(N_DP, dtype=jnp.int32))
    return (results[0].reshape(TOKENS, HEADS * HEAD_DIM), results[1].reshape(TOKENS, D))
```

```python
import functools

import jax
import jax.numpy as jnp
from jax import lax
from jax.experimental import pallas as pl
from jax.experimental.pallas import tpu as pltpu
from jax.sharding import PartitionSpec as P

D = 8192
HEADS = 64
KV_HEADS = 8
HEAD_DIM = 128


EPSILON = 1e-06
ROPE_BASE = 1000000.0


def packing(length_row, row_count):
    starts = jnp.cumsum(length_row) - length_row
    places = jnp.arange(row_count, dtype=jnp.int32)
    segment = jnp.sum((places[:, None] >= starts[None, 1:]).astype(jnp.int32), axis=1)
    onehot = (segment[:, None] == jnp.arange(length_row.shape[0], dtype=jnp.int32)[None, :]).astype(
        jnp.int32
    )
    offset = places - jnp.sum(onehot * starts[None, :], axis=1)
    return (segment, offset, onehot)


def tables(offset, head_width):
    halfway = head_width // 2
    frequency = ROPE_BASE ** (-2.0 * jnp.arange(halfway, dtype=jnp.float32) / head_width)
    angles = offset.astype(jnp.float32)[:, None] * frequency[None, :]
    angles = jnp.concatenate([angles, angles], axis=1)
    return (jnp.cos(angles)[:, None, :], jnp.sin(angles)[:, None, :])


def rotate(values, cosine, sine_table):
    halfway = values.shape[-1] // 2
    turned = jnp.concatenate([-values[..., halfway:], values[..., :halfway]], axis=-1)
    return values * cosine + turned * sine_table


def unrotate(gradient, cosine, sine_table):
    halfway = gradient.shape[-1] // 2
    scaled = gradient * sine_table
    turned = jnp.concatenate([scaled[..., halfway:], -scaled[..., :halfway]], axis=-1)
    return gradient * cosine + turned


def normalize(hidden, norm_gain):
    widened = hidden.astype(jnp.float32)
    inverse = lax.rsqrt(jnp.mean(widened * widened, axis=1) + EPSILON)
    normed = (widened * inverse[:, None] * norm_gain).astype(jnp.bfloat16)
    return (widened, inverse, normed)


def masked_softmax(scores, allowed):
    scores = jnp.where(allowed, scores, -1e30)
    highest = jnp.max(scores, axis=-1, keepdims=True)
    exponent = jnp.where(allowed, jnp.exp(scores - highest), 0.0)
    return exponent / jnp.sum(exponent, axis=-1, keepdims=True)


def contract_last(operand, weights):
    return lax.dot_general(
        operand, weights, (((1,), (1,)), ((), ())), preferred_element_type=jnp.float32
    )


def on_device(
    hidden_slots,
    lengths,
    owners,
    norm_gain,
    w_query,
    query_bias,
    w_keyvalue,
    keyvalue_bias,
    grad_attention,
):
    slot_count, window, feature_part = hidden_slots.shape
    owner_count = lax.axis_size("dp")
    dp_index = lax.axis_index("dp")
    picked = (owners == dp_index).astype(jnp.bfloat16)
    outgoing = jnp.einsum(
        "bj,jld->bld", picked, hidden_slots, preferred_element_type=jnp.float32
    ).astype(jnp.bfloat16)
    arrived = lax.all_to_all(outgoing, "dp", split_axis=0, concat_axis=0, tiled=True)
    row_count = grad_attention.shape[0]
    length_row = lax.dynamic_index_in_dim(lengths, dp_index, 0, keepdims=False)
    owner_row = lax.dynamic_index_in_dim(owners, dp_index, 0, keepdims=False)
    segment, offset, onehot = packing(length_row, row_count)
    source = jnp.sum(onehot * owner_row[None, :], axis=1)
    row_index = source * window + offset
    local_rows = jnp.take(arrived.reshape(owner_count * window, feature_part), row_index, axis=0)
    full_rows = lax.all_gather(local_rows, "tensor", axis=1, tiled=True)
    widened, inverse, normed = normalize(full_rows, norm_gain)
    tensor_index = lax.axis_index("tensor")
    lane_count = lax.axis_size("tensor")
    column_start = tensor_index * feature_part
    normed_local = lax.dynamic_slice_in_dim(normed, column_start, feature_part, 1)
    query_full = jnp.dot(normed, w_query, preferred_element_type=jnp.float32) + query_bias
    partial_kv = jnp.dot(normed_local, w_keyvalue, preferred_element_type=jnp.float32)
    keyvalue = lax.psum(partial_kv, "tensor") + keyvalue_bias
    local_heads = w_query.shape[1] // HEAD_DIM
    kv_width = KV_HEADS * HEAD_DIM
    half_dim = HEAD_DIM // 2
    score_scale = HEAD_DIM ** (-0.5)
    group_index = tensor_index * local_heads // (HEADS // KV_HEADS)
    key_start = group_index * HEAD_DIM
    cosine, sine_table = tables(offset, HEAD_DIM)
    query_rot = rotate(
        query_full.reshape(row_count, local_heads, HEAD_DIM), cosine, sine_table
    ).astype(jnp.bfloat16)
    key_rot = rotate(
        lax.dynamic_slice_in_dim(keyvalue, key_start, HEAD_DIM, 1), cosine[:, 0], sine_table[:, 0]
    ).astype(jnp.bfloat16)
    value_one = lax.dynamic_slice_in_dim(keyvalue, kv_width + key_start, HEAD_DIM, 1).astype(
        jnp.bfloat16
    )
    places = jnp.arange(row_count, dtype=jnp.int32)
    allowed = (segment[:, None] == segment[None, :]) & (places[None, :] <= places[:, None])
    scores = (
        jnp.einsum("qhd,kd->hqk", query_rot, key_rot, preferred_element_type=jnp.float32)
        * score_scale
    )
    attn_weights = masked_softmax(scores, allowed[None])
    low_weights = attn_weights.astype(jnp.bfloat16)
    attended = jnp.einsum(
        "hqk,kd->qhd", low_weights, value_one, preferred_element_type=jnp.float32
    ).astype(jnp.bfloat16)
    upstream = grad_attention.reshape(row_count, local_heads, HEAD_DIM)
    weight_grad = jnp.einsum("qhd,kd->hqk", upstream, value_one, preferred_element_type=jnp.float32)
    value_grad = jnp.einsum(
        "hqk,qhd->kd", low_weights, upstream, preferred_element_type=jnp.float32
    )
    row_inner = jnp.sum(attn_weights * weight_grad, axis=-1, keepdims=True)
    score_grad = (attn_weights * (weight_grad - row_inner) * score_scale).astype(jnp.bfloat16)
    query_grad = unrotate(
        jnp.einsum("hqk,kd->qhd", score_grad, key_rot, preferred_element_type=jnp.float32),
        cosine,
        sine_table,
    ).astype(jnp.bfloat16)
    key_grad = jnp.einsum("hqk,qhd->kd", score_grad, query_rot, preferred_element_type=jnp.float32)
    zeros_kv = jnp.zeros((row_count, 2 * kv_width), jnp.float32)
    partial_grad = lax.dynamic_update_slice_in_dim(zeros_kv, key_grad, key_start, 1)
    partial_grad = lax.dynamic_update_slice_in_dim(
        partial_grad, value_grad, kv_width + key_start, 1
    )
    paired = (
        partial_grad.reshape(row_count, 2, KV_HEADS, 2, half_dim)
        .transpose(0, 1, 2, 4, 3)
        .reshape(row_count, 2 * kv_width)
    )
    share_width = 2 * kv_width // lane_count
    shared = lax.psum_scatter(paired, "tensor", scatter_dimension=1, tiled=True)
    position = tensor_index * share_width + jnp.arange(share_width // 2, dtype=jnp.int32) * 2
    frequency_index = position // 2 % half_dim
    is_key = (position < kv_width).astype(jnp.float32)
    frequency = ROPE_BASE ** (-2.0 * frequency_index.astype(jnp.float32) / HEAD_DIM)
    angles = offset.astype(jnp.float32)[:, None] * frequency[None, :]
    cos_pair = is_key[None, :] * jnp.cos(angles) + (1.0 - is_key[None, :])
    sin_pair = is_key[None, :] * jnp.sin(angles)
    pairs = shared.reshape(row_count, share_width // 2, 2)
    first_half = pairs[:, :, 0] * cos_pair + pairs[:, :, 1] * sin_pair
    second_half = pairs[:, :, 1] * cos_pair - pairs[:, :, 0] * sin_pair
    finished = (
        jnp.stack([first_half, second_half], axis=2)
        .reshape(row_count, share_width)
        .astype(jnp.bfloat16)
    )
    gathered = lax.all_gather(finished, "tensor", axis=1, tiled=True)
    kv_grad = (
        gathered.reshape(row_count, 2, KV_HEADS, half_dim, 2)
        .transpose(0, 1, 2, 4, 3)
        .reshape(row_count, 2 * kv_width)
    )
    query_flat = query_grad.reshape(row_count, local_heads * HEAD_DIM)
    query_part = contract_last(query_flat, w_query)
    normed_grad = lax.psum_scatter(
        query_part.astype(jnp.bfloat16), "tensor", scatter_dimension=1, tiled=True
    ).astype(jnp.float32) + contract_last(kv_grad, w_keyvalue)
    gain_local = lax.dynamic_slice_in_dim(norm_gain, column_start, feature_part, 0)
    hidden_local = local_rows.astype(jnp.float32)
    scaled = gain_local * normed_grad
    row_stat = lax.psum(jnp.sum(scaled * hidden_local, axis=1), "tensor") / D
    input_grad = (
        inverse[:, None] * scaled - hidden_local * (inverse**3 * row_stat)[:, None]
    ).astype(jnp.bfloat16)
    return (attended.reshape(row_count, local_heads * HEAD_DIM), input_grad)


def call(kernel, out, ins, scratch=(), flops=0, moved=0):
    return pl.pallas_call(
        kernel,
        out_shape=[jax.ShapeDtypeStruct(shape, kind) for shape, kind in out],
        in_specs=[pl.BlockSpec(memory_space=space) for _, space in ins],
        out_specs=[pl.BlockSpec(memory_space=pltpu.VMEM) for _ in out],
        scratch_shapes=list(scratch),
        compiler_params=pltpu.CompilerParams(vmem_limit_bytes=48 * 1024 * 1024),
        cost_estimate=pl.CostEstimate(flops=flops, bytes_accessed=moved, transcendentals=0),
    )(*[array for array, _ in ins])


SMEM, VMEM, ANY = pltpu.SMEM, pltpu.VMEM, pl.ANY


def pack_kernel(table_ref, length_ref, owner_ref, *refs):
    windows, out_ref = refs[:-1], refs[-1]
    count, me = len(windows), table_ref[0]
    rows, width = out_ref.shape[0], windows[0].shape[0]
    place = lax.broadcasted_iota(jnp.int32, (rows, width), 0)
    inner = lax.broadcasted_iota(jnp.int32, (rows, width), 1)
    begin = jnp.int32(0)
    starts, sizes = [jnp.int32(0)] * count, [jnp.int32(0)] * count
    for j in range(count):
        size = length_ref[me, j]
        shift = lax.rem(me - owner_ref[me, j] + count, count)
        for k in range(count):
            starts[k] = jnp.where(shift == k, begin, starts[k])
            sizes[k] = jnp.where(shift == k, size, sizes[k])
        begin = begin + size
    total = jnp.zeros(out_ref.shape, jnp.float32)
    for k in range(count):
        chosen = ((place - starts[k]) == inner) & (inner < sizes[k])
        total += jnp.dot(
            jnp.where(chosen, 1.0, 0.0).astype(jnp.bfloat16),
            windows[k][...],
            preferred_element_type=jnp.float32,
        )
    out_ref[...] = total.astype(jnp.bfloat16)


def gained(piece, gain):
    return (piece.astype(jnp.float32) * gain).astype(jnp.bfloat16)


def keyvalue_kernel(heads, table_ref, x_ref, gain_ref, w_ref, keep_ref, send_ref, buffer, sems):
    me = table_ref[1]
    half = len(heads) * HEAD_DIM

    def copies(i):
        head = me ^ heads[i]
        return [
            pltpu.make_async_copy(
                w_ref.at[:, pl.ds(pl.multiple_of(part * half + head * HEAD_DIM, HEAD_DIM), HEAD_DIM)],
                buffer.at[i, part],
                sems.at[i, part],
            )
            for part in range(2)
        ]

    for i in range(len(heads)):
        for copy in copies(i):
            copy.start()
    scaled = gained(x_ref[...], gain_ref[me])
    for i in range(len(heads)):
        for copy in copies(i):
            copy.wait()
        both = jnp.concatenate([buffer[i, 0], buffer[i, 1]], axis=1)
        product = jnp.dot(scaled, both, preferred_element_type=jnp.float32).astype(jnp.bfloat16)
        if heads[i] & 1:
            send_ref[heads[i] >> 1] = product
        else:
            keep_ref[heads[i] >> 1] = product


def query_kernel(offset, count, first, table_ref, *refs):
    pieces, refs = refs[:count], refs[count:]
    gain_ref, w_ref, refs = refs[0], refs[1], refs[2:]
    if not first:
        acc_in, square_in, refs = refs[0], refs[1], refs[2:]
    acc_ref, square_ref, x_buffer, w_buffer, x_sems, w_sems = refs
    depth = x_buffer.shape[2]

    def w_copy(i):
        start = pl.multiple_of(table_ref[offset + i] * depth, depth)
        return pltpu.make_async_copy(w_ref.at[pl.ds(start, depth)], w_buffer.at[i], w_sems.at[i])

    def x_copy(i):
        return pltpu.make_async_copy(pieces[i], x_buffer.at[i], x_sems.at[i])

    for i in range(count):
        x_copy(i).start()
        w_copy(i).start()
    for i in range(count):
        x_copy(i).wait()
        wide = x_buffer[i].astype(jnp.float32)
        squares = wide * wide
        folded = squares[:, :HEAD_DIM]
        for k in range(1, depth // HEAD_DIM):
            folded += squares[:, k * HEAD_DIM : (k + 1) * HEAD_DIM]
        scaled = (wide * gain_ref[table_ref[offset + i]]).astype(jnp.bfloat16)
        w_copy(i).wait()
        product = jnp.dot(scaled, w_buffer[i], preferred_element_type=jnp.float32)
        if i == 0:
            acc_ref[...] = product if first else acc_in[...] + product
            square_ref[...] = folded if first else square_in[...] + folded
        else:
            acc_ref[...] += product
            square_ref[...] += folded


def dot_nt(left, right):
    return lax.dot_general(left, right, (((1,), (1,)), ((), ())), preferred_element_type=jnp.float32)


def dot_tn(left, right):
    return lax.dot_general(left, right, (((0,), (0,)), ((), ())), preferred_element_type=jnp.float32)


def attention_kernel(
    width,
    table_ref,
    length_ref,
    acc_ref,
    square_ref,
    own_kv,
    x_kv,
    y_kv,
    d_kv,
    cos_ref,
    sin_ref,
    bias_ref,
    kv_bias_ref,
    upstream_ref,
    attended_ref,
    query_grad_ref,
    kv_grad_ref,
    inverse_ref,
):
    rows = acc_ref.shape[0]
    heads = acc_ref.shape[1] // HEAD_DIM
    me, block = table_ref[0], table_ref[1]
    scale = HEAD_DIM ** (-0.5)
    inverse = lax.rsqrt(jnp.sum(square_ref[...], axis=1, keepdims=True) / width + EPSILON)
    cosine, sine = cos_ref[...], sin_ref[...]

    def rot(u):
        return u * cosine + pltpu.roll(u, HEAD_DIM // 2, 1) * sine

    def unrot(z):
        return z * cosine - pltpu.roll(z, HEAD_DIM // 2, 1) * sine

    kv_acc = sum(part[...].astype(jnp.float32) for part in (own_kv, x_kv, y_kv, d_kv))
    key_acc, value_acc = kv_acc[:, :HEAD_DIM], kv_acc[:, HEAD_DIM:]
    key = rot(key_acc * inverse + kv_bias_ref[block]).astype(jnp.bfloat16)
    value = (value_acc * inverse + kv_bias_ref[KV_HEADS + block]).astype(jnp.bfloat16)
    row = lax.broadcasted_iota(jnp.int32, (rows, rows), 0)
    column = lax.broadcasted_iota(jnp.int32, (rows, rows), 1)
    wide_row = lax.broadcasted_iota(jnp.int32, (rows, 2 * HEAD_DIM), 0)
    wide_column = lax.broadcasted_iota(jnp.int32, (rows, 2 * HEAD_DIM), 1)
    row_segment = jnp.zeros((rows, rows), jnp.int32)
    column_segment = jnp.zeros((rows, rows), jnp.int32)
    begin = jnp.int32(0)
    for j in range(length_ref.shape[1] - 1):
        begin = begin + length_ref[me, j]
        row_segment += jnp.where(row >= begin, 1, 0)
        column_segment += jnp.where(column >= begin, 1, 0)
    allowed = (row_segment == column_segment) & (column <= row)
    key_grad = jnp.zeros((rows, HEAD_DIM), jnp.float32)
    value_grad = jnp.zeros((rows, HEAD_DIM), jnp.float32)
    inner = jnp.zeros((rows, HEAD_DIM), jnp.float32)
    for h in range(heads):
        part = slice(h * HEAD_DIM, (h + 1) * HEAD_DIM)
        acc = acc_ref[:, part]
        query = rot(acc * inverse + bias_ref[:, part]).astype(jnp.bfloat16)
        scores = jnp.where(allowed, dot_nt(query, key) * scale, -1e30)
        highest = jnp.max(scores, axis=1, keepdims=True)
        exponent = jnp.where(allowed, jnp.exp(scores - highest), 0.0)
        weights = exponent / jnp.sum(exponent, axis=1, keepdims=True)
        low = weights.astype(jnp.bfloat16)
        attended_ref[:, part] = jnp.dot(low, value, preferred_element_type=jnp.float32).astype(
            jnp.bfloat16
        )
        upstream = upstream_ref[:, part]
        weight_grad = dot_nt(upstream, value)
        row_inner = jnp.sum(weights * weight_grad, axis=1, keepdims=True)
        score_grad = (weights * (weight_grad - row_inner) * scale).astype(jnp.bfloat16)
        query_grad = unrot(jnp.dot(score_grad, key, preferred_element_type=jnp.float32)).astype(
            jnp.bfloat16
        )
        query_grad_ref[:, part] = query_grad
        inner += query_grad.astype(jnp.float32) * acc
        key_grad += dot_tn(score_grad, query)
        value_grad += dot_tn(low, upstream)
    key_low, value_low = unrot(key_grad).astype(jnp.bfloat16), value_grad.astype(jnp.bfloat16)
    inner += key_low.astype(jnp.float32) * key_acc + value_low.astype(jnp.float32) * value_acc
    kv_grad_ref[:rows, :HEAD_DIM] = key_low
    kv_grad_ref[:rows, HEAD_DIM:] = value_low
    column_sum = jnp.sum(inner, axis=1, keepdims=True)
    as_row = jnp.sum(jnp.where(wide_row == wide_column, column_sum, 0.0), axis=0, keepdims=True)
    high = as_row.astype(jnp.bfloat16)
    rest = as_row - high.astype(jnp.float32)
    middle = rest.astype(jnp.bfloat16)
    last = (rest - middle.astype(jnp.float32)).astype(jnp.bfloat16)
    extra = kv_grad_ref.shape[0] - rows
    index = lax.broadcasted_iota(jnp.int32, (extra, 2 * HEAD_DIM), 0)
    tail = jnp.where(index == 0, high.astype(jnp.float32), 0.0)
    tail = jnp.where(index == 1, middle.astype(jnp.float32), tail)
    tail = jnp.where(index == 2, last.astype(jnp.float32), tail)
    kv_grad_ref[rows:, :] = tail.astype(jnp.bfloat16)
    inverse_ref[...] = jnp.broadcast_to(inverse, inverse_ref.shape)


def gradient_kernel(offset, count, table_ref, grad_ref, w_ref, *refs):
    outs, w_buffer, sems = refs[:count], refs[count], refs[count + 1]
    depth = w_buffer.shape[1]

    def w_copy(i):
        start = pl.multiple_of(table_ref[offset + i] * depth, depth)
        return pltpu.make_async_copy(w_ref.at[pl.ds(start, depth)], w_buffer.at[i], sems.at[i])

    for i in range(count):
        w_copy(i).start()
    for i in range(count):
        w_copy(i).wait()
        outs[i][...] = dot_nt(grad_ref[...], w_buffer[i]).astype(jnp.bfloat16)


def keyvalue_gradient_kernel(rows, table_ref, *refs):
    pieces, (w_ref, out_ref, inner_ref, joined) = refs[:-4], refs[-4:]
    count = len(pieces)
    half = count * HEAD_DIM
    tail = jnp.zeros((pieces[0].shape[0] - rows, 2 * HEAD_DIM), jnp.float32)
    for i in range(count):
        head = table_ref[2 + i]
        for part in range(2):
            start = pl.multiple_of(part * half + head * HEAD_DIM, HEAD_DIM)
            joined[:, pl.ds(start, HEAD_DIM)] = pieces[i][
                :rows, part * HEAD_DIM : (part + 1) * HEAD_DIM
            ]
        tail += pieces[i][rows:, :].astype(jnp.float32)
    out_ref[...] = dot_nt(joined[...], w_ref[...])
    as_row = jnp.sum(tail, axis=0, keepdims=True)
    row = lax.broadcasted_iota(jnp.int32, (rows, 2 * HEAD_DIM), 0)
    column = lax.broadcasted_iota(jnp.int32, (rows, 2 * HEAD_DIM), 1)
    as_column = jnp.sum(jnp.where(row == column, as_row, 0.0), axis=1, keepdims=True)
    inner_ref[...] = jnp.broadcast_to(as_column, inner_ref.shape)


def finish_kernel(
    width, table_ref, mine_ref, other_ref, last_ref, kv_ref, inner_ref, inverse_ref, x_ref, gain_ref, out_ref
):
    normed_grad = kv_ref[...]
    for part in (mine_ref, other_ref, last_ref):
        normed_grad += part[...].astype(jnp.float32)
    inverse = inverse_ref[:, :1]
    factor = inverse * inverse * inverse * (inner_ref[:, :1] / width)
    out_ref[...] = (
        inverse * (gain_ref[table_ref[1]] * normed_grad) - x_ref[...].astype(jnp.float32) * factor
    ).astype(jnp.bfloat16)


def cube_device(
    hidden_slots,
    lengths,
    owners,
    norm_gain,
    w_query,
    query_bias,
    w_keyvalue,
    keyvalue_bias,
    grad_attention,
):
    window, depth = hidden_slots.shape[1:]
    owner_count, lane_count = lax.axis_size("dp"), lax.axis_size("tensor")
    rows, columns = grad_attention.shape
    width = depth * lane_count
    dp_index, block = lax.axis_index("dp"), lax.axis_index("tensor")
    half, full = jnp.bfloat16, jnp.float32

    def swap(value):
        return lax.ppermute(value, "tensor", [(i, i ^ 1) for i in range(lane_count)])

    def near(value):
        return lax.ppermute(value, "tensor", [(i, i ^ (4 if i & 1 else 2)) for i in range(lane_count)])

    def far(value):
        return lax.ppermute(value, "tensor", [(i, i ^ (2 if i & 1 else 4)) for i in range(lane_count)])

    def flip(value, distance):
        return lax.ppermute(value, "tensor", [(i, i ^ distance) for i in range(lane_count)])

    apart = jnp.where(
        block & 1 == 1,
        jnp.array([0, 1, 4, 5, 3, 2, 6, 7], jnp.int32),
        jnp.array([0, 1, 2, 3, 5, 4, 6, 7], jnp.int32),
    )
    table = jnp.concatenate([jnp.stack([dp_index, block]).astype(jnp.int32), block ^ apart])
    own, a0_at, a1_at, c_at = 2, 4, 5, 8

    arrived = []
    for shift in range(owner_count):
        target = lax.rem(dp_index + shift, owner_count)
        picked = lax.dynamic_index_in_dim(owners, target, 0, keepdims=False) == dp_index
        slot = jnp.sum(jnp.where(picked, jnp.arange(owner_count, dtype=jnp.int32), 0))
        rollout = lax.dynamic_index_in_dim(hidden_slots, slot, 0, keepdims=False)
        if shift:
            pairs = [(i, (i + shift) % owner_count) for i in range(owner_count)]
            rollout = lax.ppermute(rollout, "dp", pairs)
        arrived.append(rollout)
    (local,) = call(
        pack_kernel,
        [((rows, depth), half)],
        [(table, SMEM), (lengths, SMEM), (owners, SMEM)] + [(piece, VMEM) for piece in arrived],
        flops=2 * rows * window * owner_count * depth,
        moved=4 * rows * depth * 2,
    )

    mate, a0 = swap(local), near(local)
    b0, c0 = swap(a0), far(a0)
    a1 = near(mate)
    b1, c1 = swap(a1), swap(c0)

    gain = norm_gain.reshape(lane_count, 1, depth)
    heads = tuple(range(lane_count))
    kv_shape = (lane_count // 2, rows, 2 * HEAD_DIM)
    keep, send = call(
        functools.partial(keyvalue_kernel, heads),
        [(kv_shape, half), (kv_shape, half)],
        [(table, SMEM), (local, VMEM), (gain, VMEM), (w_keyvalue, ANY)],
        scratch=[
            pltpu.VMEM((lane_count, 2, depth, HEAD_DIM), half),
            pltpu.SemaphoreType.DMA((lane_count, 2)),
        ],
        flops=2 * rows * depth * w_keyvalue.shape[1],
        moved=w_keyvalue.size * 2,
    )
    other = swap(send)
    kv_parts = []
    for chip in range(lane_count // 2):
        both = (keep[chip].astype(full) + other[chip].astype(full)).astype(half)
        kv_parts.append(flip(both, 2 * chip) if chip else both)

    def query(offset, pieces, before):
        count = len(pieces)
        return call(
            functools.partial(query_kernel, offset, count, before is None),
            [((rows, columns), full), ((rows, HEAD_DIM), full)],
            [(table, SMEM)]
            + [(piece, ANY) for piece in pieces]
            + [(gain, VMEM), (w_query, ANY)]
            + ([] if before is None else [(value, VMEM) for value in before]),
            scratch=[
                pltpu.VMEM((count, rows, depth), half),
                pltpu.VMEM((count, depth, columns), half),
                pltpu.SemaphoreType.DMA((count,)),
                pltpu.SemaphoreType.DMA((count,)),
            ],
            flops=2 * rows * depth * columns * count,
            moved=count * depth * columns * 2,
        )

    sums = query(2, [local, mate], None)
    sums = query(4, [a0, a1, b0, b1], sums)
    acc, square = query(8, [c0, c1], sums)

    _, offset, _ = packing(lax.dynamic_index_in_dim(lengths, dp_index, 0, keepdims=False), rows)
    cosine, sine = tables(offset, HEAD_DIM)
    sign = jnp.where(jnp.arange(HEAD_DIM) < HEAD_DIM // 2, -1.0, 1.0)
    extra = 16
    attended, query_grad, kv_grad, inverse = call(
        functools.partial(attention_kernel, width),
        [
            ((rows, columns), half),
            ((rows, columns), half),
            ((rows + extra, 2 * HEAD_DIM), half),
            ((rows, HEAD_DIM), full),
        ],
        [(table, SMEM), (lengths, SMEM), (acc, VMEM), (square, VMEM)]
        + [(part, VMEM) for part in kv_parts]
        + [
            (cosine[:, 0], VMEM),
            (sine[:, 0] * sign, VMEM),
            (query_bias.reshape(1, columns), VMEM),
            (keyvalue_bias.reshape(2 * KV_HEADS, 1, HEAD_DIM), VMEM),
            (grad_attention, VMEM),
        ],
        flops=14 * rows * rows * columns,
        moved=rows * columns * 10,
    )

    kv_mate, kv_a0 = swap(kv_grad), near(kv_grad)
    kv_b0, kv_c0 = swap(kv_a0), far(kv_a0)
    kv_a1 = near(kv_mate)
    kv_b1, kv_c1 = swap(kv_a1), swap(kv_c0)
    kv_all = [kv_grad, kv_mate, kv_a0, kv_a1, kv_b0, kv_b1, kv_c0, kv_c1]
    kv_normed, inner = call(
        functools.partial(keyvalue_gradient_kernel, rows),
        [((rows, depth), full), ((rows, HEAD_DIM), full)],
        [(table, SMEM)] + [(piece, VMEM) for piece in kv_all] + [(w_keyvalue, VMEM)],
        scratch=[pltpu.VMEM((rows, w_keyvalue.shape[1]), half)],
        flops=2 * rows * depth * w_keyvalue.shape[1],
        moved=w_keyvalue.size * 2,
    )

    def gradient(offset, count):
        return call(
            functools.partial(gradient_kernel, offset, count),
            [((rows, depth), half)] * count,
            [(table, SMEM), (query_grad, VMEM), (w_query, ANY)],
            scratch=[pltpu.VMEM((count, depth, columns), half), pltpu.SemaphoreType.DMA((count,))],
            flops=2 * rows * depth * columns * count,
            moved=count * depth * columns * 2,
        )

    def added(*parts):
        return sum(part.astype(full) for part in parts).astype(half)

    to_c0, to_c1 = gradient(8, 2)
    from_far = far(added(swap(to_c1), to_c0))
    to_b0, to_b1 = gradient(6, 2)
    to_a0, to_a1 = gradient(4, 2)
    to_own, to_mate = gradient(2, 2)
    near_mate = near(added(swap(to_b1), to_a1))
    near_own = near(added(swap(to_b0), to_a0, from_far))
    from_mate = swap(added(to_mate, near_mate))
    (input_grad,) = call(
        functools.partial(finish_kernel, width),
        [((rows, depth), half)],
        [(table, SMEM)]
        + [(part, VMEM) for part in (to_own, from_mate, near_own, kv_normed, inner, inverse, local, gain)],
        flops=8 * rows * depth,
        moved=rows * depth * 14,
    )
    return attended, input_grad


def solution(mesh):
    in_specs = (
        P("dp", None, "tensor"),
        P(),
        P(),
        P(),
        P(None, "tensor"),
        P("tensor"),
        P("tensor", None),
        P(),
        P("dp", "tensor"),
    )
    out_specs = (P("dp", "tensor"), P("dp", "tensor"))
    cube = mesh.shape["tensor"] == 8 and KV_HEADS == 8
    return jax.shard_map(
        cube_device if cube else on_device, mesh=mesh, in_specs=in_specs, out_specs=out_specs, check_vma=False
    )
```

```python
import functools

import jax
import jax.numpy as jnp
from jax import lax
from jax.experimental import pallas as pl
from jax.experimental.pallas import tpu as pltpu
from jax.sharding import PartitionSpec as P

D = 8192
HEADS = 64
KV_HEADS = 8
HEAD_DIM = 128


EPSILON = 1e-06
ROPE_BASE = 1000000.0


def packing(length_row, row_count):
    starts = jnp.cumsum(length_row) - length_row
    places = jnp.arange(row_count, dtype=jnp.int32)
    segment = jnp.sum((places[:, None] >= starts[None, 1:]).astype(jnp.int32), axis=1)
    onehot = (segment[:, None] == jnp.arange(length_row.shape[0], dtype=jnp.int32)[None, :]).astype(
        jnp.int32
    )
    offset = places - jnp.sum(onehot * starts[None, :], axis=1)
    return (segment, offset, onehot)


def tables(offset, head_width):
    halfway = head_width // 2
    frequency = ROPE_BASE ** (-2.0 * jnp.arange(halfway, dtype=jnp.float32) / head_width)
    angles = offset.astype(jnp.float32)[:, None] * frequency[None, :]
    angles = jnp.concatenate([angles, angles], axis=1)
    return (jnp.cos(angles)[:, None, :], jnp.sin(angles)[:, None, :])


def rotate(values, cosine, sine_table):
    halfway = values.shape[-1] // 2
    turned = jnp.concatenate([-values[..., halfway:], values[..., :halfway]], axis=-1)
    return values * cosine + turned * sine_table


def unrotate(gradient, cosine, sine_table):
    halfway = gradient.shape[-1] // 2
    scaled = gradient * sine_table
    turned = jnp.concatenate([scaled[..., halfway:], -scaled[..., :halfway]], axis=-1)
    return gradient * cosine + turned


def normalize(hidden, norm_gain):
    widened = hidden.astype(jnp.float32)
    inverse = lax.rsqrt(jnp.mean(widened * widened, axis=1) + EPSILON)
    normed = (widened * inverse[:, None] * norm_gain).astype(jnp.bfloat16)
    return (widened, inverse, normed)


def masked_softmax(scores, allowed):
    scores = jnp.where(allowed, scores, -1e30)
    highest = jnp.max(scores, axis=-1, keepdims=True)
    exponent = jnp.where(allowed, jnp.exp(scores - highest), 0.0)
    return exponent / jnp.sum(exponent, axis=-1, keepdims=True)


def contract_last(operand, weights):
    return lax.dot_general(
        operand, weights, (((1,), (1,)), ((), ())), preferred_element_type=jnp.float32
    )


def on_device(
    hidden_slots,
    lengths,
    owners,
    norm_gain,
    w_query,
    query_bias,
    w_keyvalue,
    keyvalue_bias,
    grad_attention,
):
    _, window, feature_part = hidden_slots.shape
    owner_count = lax.axis_size("dp")
    dp_index = lax.axis_index("dp")
    picked = (owners == dp_index).astype(jnp.bfloat16)
    outgoing = jnp.einsum(
        "bj,jld->bld", picked, hidden_slots, preferred_element_type=jnp.float32
    ).astype(jnp.bfloat16)
    arrived = lax.all_to_all(outgoing, "dp", split_axis=0, concat_axis=0, tiled=True)
    row_count = grad_attention.shape[0]
    length_row = lax.dynamic_index_in_dim(lengths, dp_index, 0, keepdims=False)
    owner_row = lax.dynamic_index_in_dim(owners, dp_index, 0, keepdims=False)
    segment, offset, onehot = packing(length_row, row_count)
    source = jnp.sum(onehot * owner_row[None, :], axis=1)
    row_index = source * window + offset
    local_rows = jnp.take(arrived.reshape(owner_count * window, feature_part), row_index, axis=0)
    full_rows = lax.all_gather(local_rows, "tensor", axis=1, tiled=True)
    _, inverse, normed = normalize(full_rows, norm_gain)
    tensor_index = lax.axis_index("tensor")
    lane_count = lax.axis_size("tensor")
    column_start = tensor_index * feature_part
    normed_local = lax.dynamic_slice_in_dim(normed, column_start, feature_part, 1)
    query_full = jnp.dot(normed, w_query, preferred_element_type=jnp.float32) + query_bias
    partial_kv = jnp.dot(normed_local, w_keyvalue, preferred_element_type=jnp.float32)
    keyvalue = lax.psum(partial_kv, "tensor") + keyvalue_bias
    local_heads = w_query.shape[1] // HEAD_DIM
    kv_width = KV_HEADS * HEAD_DIM
    half_dim = HEAD_DIM // 2
    score_scale = HEAD_DIM ** (-0.5)
    group_index = tensor_index * local_heads // (HEADS // KV_HEADS)
    key_start = group_index * HEAD_DIM
    cosine, sine_table = tables(offset, HEAD_DIM)
    query_rot = rotate(
        query_full.reshape(row_count, local_heads, HEAD_DIM), cosine, sine_table
    ).astype(jnp.bfloat16)
    key_rot = rotate(
        lax.dynamic_slice_in_dim(keyvalue, key_start, HEAD_DIM, 1), cosine[:, 0], sine_table[:, 0]
    ).astype(jnp.bfloat16)
    value_one = lax.dynamic_slice_in_dim(keyvalue, kv_width + key_start, HEAD_DIM, 1).astype(
        jnp.bfloat16
    )
    places = jnp.arange(row_count, dtype=jnp.int32)
    allowed = (segment[:, None] == segment[None, :]) & (places[None, :] <= places[:, None])
    scores = (
        jnp.einsum("qhd,kd->hqk", query_rot, key_rot, preferred_element_type=jnp.float32)
        * score_scale
    )
    attn_weights = masked_softmax(scores, allowed[None])
    low_weights = attn_weights.astype(jnp.bfloat16)
    attended = jnp.einsum(
        "hqk,kd->qhd", low_weights, value_one, preferred_element_type=jnp.float32
    ).astype(jnp.bfloat16)
    upstream = grad_attention.reshape(row_count, local_heads, HEAD_DIM)
    weight_grad = jnp.einsum("qhd,kd->hqk", upstream, value_one, preferred_element_type=jnp.float32)
    value_grad = jnp.einsum(
        "hqk,qhd->kd", low_weights, upstream, preferred_element_type=jnp.float32
    )
    row_inner = jnp.sum(attn_weights * weight_grad, axis=-1, keepdims=True)
    score_grad = (attn_weights * (weight_grad - row_inner) * score_scale).astype(jnp.bfloat16)
    query_grad = unrotate(
        jnp.einsum("hqk,kd->qhd", score_grad, key_rot, preferred_element_type=jnp.float32),
        cosine,
        sine_table,
    ).astype(jnp.bfloat16)
    key_grad = jnp.einsum("hqk,qhd->kd", score_grad, query_rot, preferred_element_type=jnp.float32)
    zeros_kv = jnp.zeros((row_count, 2 * kv_width), jnp.float32)
    partial_grad = lax.dynamic_update_slice_in_dim(zeros_kv, key_grad, key_start, 1)
    partial_grad = lax.dynamic_update_slice_in_dim(
        partial_grad, value_grad, kv_width + key_start, 1
    )
    paired = (
        partial_grad.reshape(row_count, 2, KV_HEADS, 2, half_dim)
        .transpose(0, 1, 2, 4, 3)
        .reshape(row_count, 2 * kv_width)
    )
    share_width = 2 * kv_width // lane_count
    shared = lax.psum_scatter(paired, "tensor", scatter_dimension=1, tiled=True)
    position = tensor_index * share_width + jnp.arange(share_width // 2, dtype=jnp.int32) * 2
    frequency_index = position // 2 % half_dim
    is_key = (position < kv_width).astype(jnp.float32)
    frequency = ROPE_BASE ** (-2.0 * frequency_index.astype(jnp.float32) / HEAD_DIM)
    angles = offset.astype(jnp.float32)[:, None] * frequency[None, :]
    cos_pair = is_key[None, :] * jnp.cos(angles) + (1.0 - is_key[None, :])
    sin_pair = is_key[None, :] * jnp.sin(angles)
    pairs = shared.reshape(row_count, share_width // 2, 2)
    first_half = pairs[:, :, 0] * cos_pair + pairs[:, :, 1] * sin_pair
    second_half = pairs[:, :, 1] * cos_pair - pairs[:, :, 0] * sin_pair
    finished = (
        jnp.stack([first_half, second_half], axis=2)
        .reshape(row_count, share_width)
        .astype(jnp.bfloat16)
    )
    gathered = lax.all_gather(finished, "tensor", axis=1, tiled=True)
    kv_grad = (
        gathered.reshape(row_count, 2, KV_HEADS, half_dim, 2)
        .transpose(0, 1, 2, 4, 3)
        .reshape(row_count, 2 * kv_width)
    )
    query_flat = query_grad.reshape(row_count, local_heads * HEAD_DIM)
    query_part = contract_last(query_flat, w_query)
    normed_grad = lax.psum_scatter(
        query_part.astype(jnp.bfloat16), "tensor", scatter_dimension=1, tiled=True
    ).astype(jnp.float32) + contract_last(kv_grad, w_keyvalue)
    gain_local = lax.dynamic_slice_in_dim(norm_gain, column_start, feature_part, 0)
    hidden_local = local_rows.astype(jnp.float32)
    scaled = gain_local * normed_grad
    row_stat = lax.psum(jnp.sum(scaled * hidden_local, axis=1), "tensor") / D
    input_grad = (
        inverse[:, None] * scaled - hidden_local * (inverse**3 * row_stat)[:, None]
    ).astype(jnp.bfloat16)
    return (attended.reshape(row_count, local_heads * HEAD_DIM), input_grad)


VMEM, HBM = pltpu.VMEM, pltpu.HBM
CHUNKS = 1
EXTRA = 16


def call(kernel, out, ins, scratch=(), flops=0, moved=0, need=8):
    return pl.pallas_call(
        kernel,
        out_shape=[pltpu.VMEM(*item) if type(item) is tuple else item for item in out],
        in_specs=[pl.BlockSpec(memory_space=space) for _, space in ins],
        out_specs=[pl.BlockSpec(memory_space=VMEM) for _ in out],
        scratch_shapes=list(scratch),
        compiler_params=pltpu.CompilerParams(vmem_limit_bytes=need * 1024 * 1024),
        cost_estimate=pl.CostEstimate(flops=flops, bytes_accessed=moved, transcendentals=0),
    )(*[pltpu.with_memory_space_constraint(array, space) for array, space in ins])


def places():
    lane = lax.axis_index("tensor")
    near = jnp.where(lane & 1 == 1, 4, 2)
    far = 6 - near
    return [lane, lane ^ 1, lane ^ near, lane ^ (near + 1), lane ^ (far + 1), lane ^ far, lane ^ 6, lane ^ 7]


OWN, MATE, A0, A1, B0, B1, C0, C1 = range(8)
PAIRS = ((OWN, MATE), (A0, B0), (A1, B1), (C0, C1))


def pick_kernel(owner_in, slots_ref, *refs):
    outs, owner_ref, sems = refs[:-2], refs[-2], refs[-1]
    read = pltpu.make_async_copy(owner_in, owner_ref, sems.at[len(outs)])
    read.start()
    read.wait()
    count, me = owner_ref.shape[0], lax.axis_index("dp")
    part = slots_ref.shape[2] // CHUNKS
    copies = []
    for shift in range(count):
        target = lax.rem(me + shift, count)
        slot = jnp.int32(0)
        for j in range(owner_ref.shape[1]):
            slot = jnp.where(owner_ref[target, j] == me, j, slot)
        for chunk in range(CHUNKS):
            i = shift * CHUNKS + chunk
            copies.append(
                pltpu.make_async_copy(
                    slots_ref.at[slot, :, pl.ds(chunk * part, part)], outs[i], sems.at[i]
                )
            )
    for copy in copies:
        copy.start()
    for copy in copies:
        copy.wait()


def prepare_kernel(
    window,
    length_in,
    owner_in,
    frequency_ref,
    kv_in,
    gain_in,
    bias_in,
    kv_bias_in,
    upstream_in,
    w_in,
    kv_ref,
    gain_ref,
    bias_ref,
    kv_bias_ref,
    upstream_ref,
    chosen_ref,
    cos_ref,
    sin_ref,
    allowed_ref,
    *refs,
):
    w_refs, (length_ref, owner_ref, sems) = refs[:-3], refs[-3:]
    reads = [
        pltpu.make_async_copy(length_in, length_ref, sems.at[0]),
        pltpu.make_async_copy(owner_in, owner_ref, sems.at[1]),
    ]
    pairs = (
        (kv_in, kv_ref),
        (gain_in, gain_ref),
        (bias_in, bias_ref),
        (kv_bias_in, kv_bias_ref),
        (upstream_in, upstream_ref),
    )
    depth = w_refs[0].shape[0]
    pairs += tuple(
        (w_in.at[pl.ds(pl.multiple_of(block * depth, depth), depth)], w_ref)
        for block, w_ref in zip(places(), w_refs)
    )
    copies = [pltpu.make_async_copy(a, b, sems.at[2 + i]) for i, (a, b) in enumerate(pairs)]
    for read in reads + copies:
        read.start()
    for read in reads:
        read.wait()
    count, me = length_ref.shape[0], lax.axis_index("dp")
    rows = cos_ref.shape[0]
    place = lax.broadcasted_iota(jnp.int32, (rows, window), 0)
    inside = lax.broadcasted_iota(jnp.int32, (rows, window), 1)
    row = lax.broadcasted_iota(jnp.int32, (rows, rows), 0)
    column = lax.broadcasted_iota(jnp.int32, (rows, rows), 1)
    row_segment = jnp.zeros((rows, rows), jnp.int32)
    column_segment = jnp.zeros((rows, rows), jnp.int32)
    position = lax.broadcasted_iota(jnp.int32, (rows, HEAD_DIM), 0)
    turn = position
    begin = jnp.int32(0)
    starts, sizes = [jnp.int32(0)] * count, [jnp.int32(0)] * count
    for j in range(count):
        size = length_ref[me, j]
        shift = lax.rem(me - owner_ref[me, j] + count, count)
        for k in range(count):
            starts[k] = jnp.where(shift == k, begin, starts[k])
            sizes[k] = jnp.where(shift == k, size, sizes[k])
        if j:
            row_segment += jnp.where(row >= begin, 1, 0)
            column_segment += jnp.where(column >= begin, 1, 0)
            turn = jnp.where(position >= begin, position - begin, turn)
        begin = begin + size
    for k in range(count):
        chosen = ((place - starts[k]) == inside) & (inside < sizes[k])
        chosen_ref[k] = jnp.where(chosen, 1.0, 0.0).astype(jnp.bfloat16)
    allowed = (row_segment == column_segment) & (column <= row)
    allowed_ref[...] = jnp.where(allowed, 1.0, 0.0)
    angle = turn.astype(jnp.float32) * frequency_ref[...]
    low_half = lax.broadcasted_iota(jnp.int32, (rows, HEAD_DIM), 1) < HEAD_DIM // 2
    cos_ref[...] = jnp.cos(angle)
    sine = jnp.sin(angle)
    sin_ref[...] = jnp.where(low_half, -sine, sine)
    for copy in copies:
        copy.wait()


def pack_kernel(chosen_ref, *refs):
    windows, out_ref = refs[:-1], refs[-1]
    total = jnp.zeros(out_ref.shape, jnp.float32)
    for k in range(len(windows)):
        total += jnp.dot(chosen_ref[k], windows[k][...], preferred_element_type=jnp.float32)
    out_ref[...] = total.astype(jnp.bfloat16)


def keyvalue_kernel(*refs):
    pieces, (gain_ref, w_ref, keep_ref, send_ref) = refs[:-4], refs[-4:]
    me = lax.axis_index("tensor")
    part = pieces[0].shape[1]
    gain = gain_ref[me]
    scaled = [
        (piece[...].astype(jnp.float32) * gain[:, i * part : (i + 1) * part]).astype(jnp.bfloat16)
        for i, piece in enumerate(pieces)
    ]
    heads = w_ref.shape[1] // (2 * HEAD_DIM)
    step = 4 * HEAD_DIM
    for start in range(0, w_ref.shape[1], step):
        product = sum(
            jnp.dot(
                scaled[i],
                w_ref[i * part : (i + 1) * part, start : start + step],
                preferred_element_type=jnp.float32,
            )
            for i in range(len(pieces))
        ).astype(jnp.bfloat16)
        for k in range(step // HEAD_DIM):
            column = start // HEAD_DIM + k
            lanes = slice(column // heads * HEAD_DIM, (column // heads + 1) * HEAD_DIM)
            apart = me ^ (column % heads)

            @pl.when(apart & 1 == 1)
            def _(k=k, lanes=lanes, apart=apart, product=product):
                send_ref[apart >> 1, :, lanes] = product[:, k * HEAD_DIM : (k + 1) * HEAD_DIM]

            @pl.when(apart & 1 == 0)
            def _(k=k, lanes=lanes, apart=apart, product=product):
                keep_ref[apart >> 1, :, lanes] = product[:, k * HEAD_DIM : (k + 1) * HEAD_DIM]


def chip_sum_kernel(keep_ref, other_ref, *outs):
    for chip, out in enumerate(outs):
        out[...] = (
            keep_ref[chip].astype(jnp.float32) + other_ref[chip].astype(jnp.float32)
        ).astype(jnp.bfloat16)


def query_kernel(names, chunk, first, *refs):
    pieces, refs = refs[: len(names)], refs[len(names) :]
    w_refs, gain_ref, refs = refs[: len(names)], refs[len(names)], refs[len(names) + 1 :]
    acc_ref, square_ref = refs[-2:]
    part = pieces[0].shape[1]
    at = places()
    squares = jnp.zeros(square_ref.shape, jnp.float32) if first else refs[1][...]
    for i, name in enumerate(names):
        wide = pieces[i][...].astype(jnp.float32)
        square = wide * wide
        for k in range(part // HEAD_DIM):
            squares += square[:, k * HEAD_DIM : (k + 1) * HEAD_DIM]
        scaled = (wide * gain_ref[at[name], :, chunk * part : (chunk + 1) * part]).astype(jnp.bfloat16)
        w_part = w_refs[i][chunk * part : (chunk + 1) * part, :]
        product = jnp.dot(scaled, w_part, preferred_element_type=jnp.float32)
        if i == 0 and not first:
            acc_ref[...] = refs[0][...] + product
        elif i == 0:
            acc_ref[...] = product
        else:
            acc_ref[...] += product
    square_ref[...] = squares


def dot_nt(left, right):
    return lax.dot_general(left, right, (((1,), (1,)), ((), ())), preferred_element_type=jnp.float32)


def dot_tn(left, right):
    return lax.dot_general(left, right, (((0,), (0,)), ((), ())), preferred_element_type=jnp.float32)


def attention_kernel(
    width,
    acc_ref,
    square_ref,
    own_kv,
    x_kv,
    y_kv,
    d_kv,
    cos_ref,
    sin_ref,
    allowed_ref,
    bias_ref,
    kv_bias_ref,
    upstream_ref,
    attended_ref,
    query_grad_ref,
    kv_grad_ref,
    inverse_ref,
):
    rows = acc_ref.shape[0]
    heads = acc_ref.shape[1] // HEAD_DIM
    block = lax.axis_index("tensor")
    scale = HEAD_DIM ** (-0.5)
    inverse = lax.rsqrt(jnp.sum(square_ref[...], axis=1, keepdims=True) / width + EPSILON)
    cosine, sine = cos_ref[...], sin_ref[...]

    def rot(u):
        return u * cosine + pltpu.roll(u, HEAD_DIM // 2, 1) * sine

    def unrot(z):
        return z * cosine - pltpu.roll(z, HEAD_DIM // 2, 1) * sine

    kv_acc = sum(part[...].astype(jnp.float32) for part in (own_kv, x_kv, y_kv, d_kv))
    key_acc, value_acc = kv_acc[:, :HEAD_DIM], kv_acc[:, HEAD_DIM:]
    key = rot(key_acc * inverse + kv_bias_ref[block]).astype(jnp.bfloat16)
    value = (value_acc * inverse + kv_bias_ref[KV_HEADS + block]).astype(jnp.bfloat16)
    allowed = allowed_ref[...] > 0.5
    key_grad = jnp.zeros((rows, HEAD_DIM), jnp.float32)
    value_grad = jnp.zeros((rows, HEAD_DIM), jnp.float32)
    inner = jnp.zeros((rows, HEAD_DIM), jnp.float32)
    for h in range(heads):
        part = slice(h * HEAD_DIM, (h + 1) * HEAD_DIM)
        acc = acc_ref[:, part]
        query = rot(acc * inverse + bias_ref[:, part]).astype(jnp.bfloat16)
        scores = jnp.where(allowed, dot_nt(query, key) * scale, -1e30)
        highest = jnp.max(scores, axis=1, keepdims=True)
        exponent = jnp.where(allowed, jnp.exp(scores - highest), 0.0)
        weights = exponent * (1.0 / jnp.sum(exponent, axis=1, keepdims=True))
        low = weights.astype(jnp.bfloat16)
        attended_ref[:, part] = jnp.dot(low, value, preferred_element_type=jnp.float32).astype(
            jnp.bfloat16
        )
        upstream = upstream_ref[:, part]
        weight_grad = dot_nt(upstream, value)
        row_inner = jnp.sum(weights * weight_grad, axis=1, keepdims=True)
        score_grad = (weights * (weight_grad - row_inner) * scale).astype(jnp.bfloat16)
        query_grad = unrot(jnp.dot(score_grad, key, preferred_element_type=jnp.float32)).astype(
            jnp.bfloat16
        )
        query_grad_ref[:, part] = query_grad
        inner += query_grad.astype(jnp.float32) * acc
        key_grad += dot_tn(score_grad, query)
        value_grad += dot_tn(low, upstream)
    key_low, value_low = unrot(key_grad).astype(jnp.bfloat16), value_grad.astype(jnp.bfloat16)
    inner += key_low.astype(jnp.float32) * key_acc + value_low.astype(jnp.float32) * value_acc
    kv_grad_ref[:rows, :HEAD_DIM] = key_low
    kv_grad_ref[:rows, HEAD_DIM:] = value_low
    row = lax.broadcasted_iota(jnp.int32, (rows, 2 * HEAD_DIM), 0)
    column = lax.broadcasted_iota(jnp.int32, (rows, 2 * HEAD_DIM), 1)
    column_sum = jnp.sum(inner, axis=1, keepdims=True)
    as_row = jnp.sum(jnp.where(row == column, column_sum, 0.0), axis=0, keepdims=True)
    high = as_row.astype(jnp.bfloat16).astype(jnp.float32)
    middle = (as_row - high).astype(jnp.bfloat16).astype(jnp.float32)
    last = as_row - high - middle
    index = lax.broadcasted_iota(jnp.int32, (EXTRA, 2 * HEAD_DIM), 0)
    tail = jnp.where(index == 0, high, 0.0)
    tail = jnp.where(index == 1, middle, tail)
    tail = jnp.where(index == 2, last, tail)
    kv_grad_ref[rows:, :] = tail.astype(jnp.bfloat16)
    inverse_ref[...] = jnp.broadcast_to(inverse, inverse_ref.shape)


def gradient_kernel(grad_ref, w_ref, *refs):
    added, out_ref = refs[:-1], refs[-1]
    total = dot_nt(grad_ref[...], w_ref[...])
    for more in added:
        total += more[...].astype(jnp.float32)
    out_ref[...] = total.astype(out_ref.dtype)


def add_kernel(left_ref, right_ref, out_ref):
    out_ref[...] = (left_ref[...] + right_ref[...].astype(jnp.float32)).astype(out_ref.dtype)


def keyvalue_gradient_kernel(*refs):
    pieces, (before_ref, w_ref, out_ref, inner_ref, joined) = refs[:-5], refs[-5:]
    rows = out_ref.shape[0]
    half = len(pieces) * HEAD_DIM
    at = places()
    tail = jnp.zeros((EXTRA, 2 * HEAD_DIM), jnp.float32)
    for i, piece in enumerate(pieces):
        for part in range(2):
            start = pl.multiple_of(part * half + at[i] * HEAD_DIM, HEAD_DIM)
            joined[:, pl.ds(start, HEAD_DIM)] = piece[:rows, part * HEAD_DIM : (part + 1) * HEAD_DIM]
        tail += piece[rows:, :].astype(jnp.float32)
    out_ref[...] = before_ref[...] + dot_nt(joined[...], w_ref[...])
    as_row = jnp.sum(tail, axis=0, keepdims=True)
    row = lax.broadcasted_iota(jnp.int32, (rows, 2 * HEAD_DIM), 0)
    column = lax.broadcasted_iota(jnp.int32, (rows, 2 * HEAD_DIM), 1)
    as_column = jnp.sum(jnp.where(row == column, as_row, 0.0), axis=1, keepdims=True)
    inner_ref[...] = jnp.broadcast_to(as_column, inner_ref.shape)


def finish_kernel(width, sum_ref, mate_ref, last_ref, inner_ref, inverse_ref, gain_ref, *refs):
    pieces, out_ref = refs[:-1], refs[-1]
    part = pieces[0].shape[1]
    inverse = inverse_ref[:, :1]
    factor = inverse * inverse * inverse * (inner_ref[:, :1] / width)
    gain = gain_ref[lax.axis_index("tensor")]
    for i, piece in enumerate(pieces):
        lanes = slice(i * part, (i + 1) * part)
        normed_grad = sum_ref[:, lanes] + mate_ref[:, lanes].astype(jnp.float32)
        normed_grad += last_ref[:, lanes].astype(jnp.float32)
        out_ref[:, lanes] = (
            inverse * (gain[:, lanes] * normed_grad) - piece[...].astype(jnp.float32) * factor
        ).astype(jnp.bfloat16)


def cube_device(
    hidden_slots,
    lengths,
    owners,
    norm_gain,
    w_query,
    query_bias,
    w_keyvalue,
    keyvalue_bias,
    grad_attention,
):
    window, depth = hidden_slots.shape[1:]
    owner_count, lane_count = lax.axis_size("dp"), lax.axis_size("tensor")
    rows, columns = grad_attention.shape
    width, part = depth * lane_count, depth // CHUNKS
    half, full = jnp.bfloat16, jnp.float32

    def permute(value, partner):
        return lax.ppermute(value, "tensor", [(i, partner(i)) for i in range(lane_count)])

    def swap(value):
        return permute(value, lambda i: i ^ 1)

    def near(value):
        return permute(value, lambda i: i ^ (4 if i & 1 else 2))

    def far(value):
        return permute(value, lambda i: i ^ (2 if i & 1 else 4))

    windows = call(
        pick_kernel,
        [((window, part), half)] * (owner_count * CHUNKS),
        [(owners, HBM), (hidden_slots, HBM)],
        scratch=[
            pltpu.SMEM(owners.shape, jnp.int32),
            pltpu.SemaphoreType.DMA((owner_count * CHUNKS + 1,)),
        ],
        moved=4 * hidden_slots.size,
    )
    arrived = [[windows[chunk]] for chunk in range(CHUNKS)]
    for chunk in range(CHUNKS):
        for shift in range(1, owner_count):
            pairs = [(i, (i + shift) % owner_count) for i in range(owner_count)]
            arrived[chunk].append(lax.ppermute(windows[shift * CHUNKS + chunk], "dp", pairs))
    frequency = ROPE_BASE ** (-2.0 * jnp.arange(HEAD_DIM // 2, dtype=full) / HEAD_DIM)
    frequency = jnp.concatenate([frequency, frequency])[None]
    w_kv, gain, bias, kv_bias, upstream, chosen, cosine, sine, allowed, *w = call(
        functools.partial(prepare_kernel, window),
        [
            (w_keyvalue.shape, half),
            ((lane_count, 1, depth), full),
            ((1, columns), full),
            ((2 * KV_HEADS, 1, HEAD_DIM), full),
            (grad_attention.shape, half),
            ((owner_count, rows, window), half),
            ((rows, HEAD_DIM), full),
            ((rows, HEAD_DIM), full),
            ((rows, rows), full),
        ]
        + [((depth, columns), half)] * lane_count,
        [
            (lengths, HBM),
            (owners, HBM),
            (frequency, VMEM),
            (w_keyvalue, HBM),
            (norm_gain.reshape(lane_count, 1, depth), HBM),
            (query_bias.reshape(1, columns), HBM),
            (keyvalue_bias.reshape(2 * KV_HEADS, 1, HEAD_DIM), HBM),
            (grad_attention, HBM),
            (w_query, HBM),
        ],
        scratch=[
            pltpu.SMEM(lengths.shape, jnp.int32),
            pltpu.SMEM(owners.shape, jnp.int32),
            pltpu.SemaphoreType.DMA((7 + lane_count,)),
        ],
        flops=64 * rows * rows,
        moved=2 * w_query.size,
        need=32,
    )
    sums = None

    def query(chunk, names, pieces):
        nonlocal sums
        sums = call(
            functools.partial(query_kernel, names, chunk, sums is None),
            [((rows, columns), full), ((rows, HEAD_DIM), full)],
            [(piece, VMEM) for piece in pieces]
            + [(w[name], VMEM) for name in names]
            + [(gain, VMEM)]
            + [(value, VMEM) for value in sums or ()],
            flops=2 * rows * part * columns * len(names),
            moved=len(names) * part * columns * 2,
        )

    local, groups = [], []
    for chunk in range(CHUNKS):
        (own,) = call(
            pack_kernel,
            [((rows, part), half)],
            [(chosen, VMEM)] + [(piece, VMEM) for piece in arrived[chunk]],
            flops=2 * rows * window * owner_count * part,
            moved=4 * rows * part * 2,
        )
        local.append(own)
        a0 = near(own)
        mate = swap(own)
        a1 = near(mate)
        b0 = swap(a0)
        c0 = far(a0)
        b1 = swap(a1)
        c1 = swap(c0)
        groups.append([own, mate, a0, a1, b0, b1, c0, c1])
    for chunk in range(CHUNKS):
        group = groups[chunk]
        for names in PAIRS:
            query(chunk, names, [group[n] for n in names])
    acc, square = sums

    kv_shape = (lane_count // 2, rows, 2 * HEAD_DIM)
    keep, send = call(
        keyvalue_kernel,
        [(kv_shape, half), (kv_shape, half)],
        [(piece, VMEM) for piece in local] + [(gain, VMEM), (w_kv, VMEM)],
        flops=2 * rows * depth * w_keyvalue.shape[1],
        moved=w_keyvalue.size * 2,
        need=16,
    )
    other = swap(send)
    kv_parts = call(
        chip_sum_kernel,
        [(kv_shape[1:], half)] * (lane_count // 2),
        [(keep, VMEM), (other, VMEM)],
        flops=rows * depth,
        moved=rows * depth * 6,
    )
    kv_parts = [kv_parts[0]] + [
        permute(kv_parts[chip], lambda i, chip=chip: i ^ (2 * chip))
        for chip in range(1, lane_count // 2)
    ]

    attended, query_grad, kv_grad, inverse = call(
        functools.partial(attention_kernel, width),
        [
            ((rows, columns), half),
            ((rows, columns), half),
            ((rows + EXTRA, 2 * HEAD_DIM), half),
            ((rows, HEAD_DIM), full),
        ],
        [(acc, VMEM), (square, VMEM)]
        + [(piece, VMEM) for piece in kv_parts]
        + [(value, VMEM) for value in (cosine, sine, allowed, bias, kv_bias, upstream)],
        flops=14 * rows * rows * columns,
        moved=rows * columns * 10,
        need=16,
    )

    def gradient(name, added=(), kind=half):
        return call(
            gradient_kernel,
            [((rows, depth), kind)],
            [(query_grad, VMEM), (w[name], VMEM)] + [(value, VMEM) for value in added],
            flops=2 * rows * depth * columns,
            moved=depth * columns * 2,
        )

    (to_c1,) = gradient(C1)
    from_c1 = swap(to_c1)
    (to_b1,) = gradient(B1)
    from_b1 = swap(to_b1)
    (to_c0,) = gradient(C0, (from_c1,))
    from_far = far(to_c0)
    (to_a1,) = gradient(A1, (from_b1,))
    near_mate = near(to_a1)
    (to_b0,) = gradient(B0)
    from_b0 = swap(to_b0)

    kv_mate, kv_a0 = swap(kv_grad), near(kv_grad)
    kv_a1 = near(kv_mate)
    kv_b0, kv_c0 = swap(kv_a0), far(kv_a0)
    kv_b1, kv_c1 = swap(kv_a1), swap(kv_c0)

    (part_a0,) = gradient(A0, (from_b0,), full)
    (to_a0,) = call(
        add_kernel,
        [((rows, depth), half)],
        [(part_a0, VMEM), (from_far, VMEM)],
        flops=rows * depth,
        moved=rows * depth * 8,
    )
    near_own = near(to_a0)
    (to_own,) = gradient(OWN, (), full)
    (to_mate,) = gradient(MATE, (near_mate,))
    from_mate = swap(to_mate)
    total, inner = call(
        keyvalue_gradient_kernel,
        [((rows, depth), full), ((rows, HEAD_DIM), full)],
        [(piece, VMEM) for piece in (kv_grad, kv_mate, kv_a0, kv_a1, kv_b0, kv_b1, kv_c0, kv_c1)]
        + [(to_own, VMEM), (w_kv, VMEM)],
        scratch=[pltpu.VMEM((rows, w_keyvalue.shape[1]), half)],
        flops=2 * rows * depth * w_keyvalue.shape[1],
        moved=w_keyvalue.size * 2,
        need=16,
    )
    (input_grad,) = call(
        functools.partial(finish_kernel, width),
        [jax.ShapeDtypeStruct((rows, depth), half)],
        [(value, VMEM) for value in (total, from_mate, near_own, inner, inverse, gain)]
        + [(piece, VMEM) for piece in local],
        flops=8 * rows * depth,
        moved=rows * depth * 14,
    )
    return attended, input_grad


def solution(mesh):
    in_specs = (
        P("dp", None, "tensor"),
        P(),
        P(),
        P(),
        P(None, "tensor"),
        P("tensor"),
        P("tensor", None),
        P(),
        P("dp", "tensor"),
    )
    out_specs = (P("dp", "tensor"), P("dp", "tensor"))
    cube = mesh.shape["tensor"] == 8 and KV_HEADS == 8

    def layer(*args):
        return cube_device(*args)

    return jax.shard_map(
        layer if cube else on_device,
        mesh=mesh,
        in_specs=in_specs,
        out_specs=out_specs,
        check_vma=False,
    )
```

```python
import functools

import jax
import jax.numpy as jnp
from jax import lax
from jax.experimental import pallas as pl
from jax.experimental.pallas import tpu as pltpu
from jax.sharding import PartitionSpec as P

D = 8192
HEADS = 64
KV_HEADS = 8
HEAD_DIM = 128


EPSILON = 1e-06
ROPE_BASE = 1000000.0


def packing(length_row, row_count):
    starts = jnp.cumsum(length_row) - length_row
    places = jnp.arange(row_count, dtype=jnp.int32)
    segment = jnp.sum((places[:, None] >= starts[None, 1:]).astype(jnp.int32), axis=1)
    onehot = (segment[:, None] == jnp.arange(length_row.shape[0], dtype=jnp.int32)[None, :]).astype(
        jnp.int32
    )
    offset = places - jnp.sum(onehot * starts[None, :], axis=1)
    return (segment, offset, onehot)


def tables(offset, head_width):
    halfway = head_width // 2
    frequency = ROPE_BASE ** (-2.0 * jnp.arange(halfway, dtype=jnp.float32) / head_width)
    angles = offset.astype(jnp.float32)[:, None] * frequency[None, :]
    angles = jnp.concatenate([angles, angles], axis=1)
    return (jnp.cos(angles)[:, None, :], jnp.sin(angles)[:, None, :])


def rotate(values, cosine, sine_table):
    halfway = values.shape[-1] // 2
    turned = jnp.concatenate([-values[..., halfway:], values[..., :halfway]], axis=-1)
    return values * cosine + turned * sine_table


def unrotate(gradient, cosine, sine_table):
    halfway = gradient.shape[-1] // 2
    scaled = gradient * sine_table
    turned = jnp.concatenate([scaled[..., halfway:], -scaled[..., :halfway]], axis=-1)
    return gradient * cosine + turned


def normalize(hidden, norm_gain):
    widened = hidden.astype(jnp.float32)
    inverse = lax.rsqrt(jnp.mean(widened * widened, axis=1) + EPSILON)
    normed = (widened * inverse[:, None] * norm_gain).astype(jnp.bfloat16)
    return (widened, inverse, normed)


def masked_softmax(scores, allowed):
    scores = jnp.where(allowed, scores, -1e30)
    highest = jnp.max(scores, axis=-1, keepdims=True)
    exponent = jnp.where(allowed, jnp.exp(scores - highest), 0.0)
    return exponent / jnp.sum(exponent, axis=-1, keepdims=True)


def contract_last(operand, weights):
    return lax.dot_general(
        operand, weights, (((1,), (1,)), ((), ())), preferred_element_type=jnp.float32
    )


def on_device(
    hidden_slots,
    lengths,
    owners,
    norm_gain,
    w_query,
    query_bias,
    w_keyvalue,
    keyvalue_bias,
    grad_attention,
):
    _, window, feature_part = hidden_slots.shape
    owner_count = lax.axis_size("dp")
    dp_index = lax.axis_index("dp")
    picked = (owners == dp_index).astype(jnp.bfloat16)
    outgoing = jnp.einsum(
        "bj,jld->bld", picked, hidden_slots, preferred_element_type=jnp.float32
    ).astype(jnp.bfloat16)
    arrived = lax.all_to_all(outgoing, "dp", split_axis=0, concat_axis=0, tiled=True)
    row_count = grad_attention.shape[0]
    length_row = lax.dynamic_index_in_dim(lengths, dp_index, 0, keepdims=False)
    owner_row = lax.dynamic_index_in_dim(owners, dp_index, 0, keepdims=False)
    segment, offset, onehot = packing(length_row, row_count)
    source = jnp.sum(onehot * owner_row[None, :], axis=1)
    row_index = source * window + offset
    local_rows = jnp.take(arrived.reshape(owner_count * window, feature_part), row_index, axis=0)
    full_rows = lax.all_gather(local_rows, "tensor", axis=1, tiled=True)
    _, inverse, normed = normalize(full_rows, norm_gain)
    tensor_index = lax.axis_index("tensor")
    lane_count = lax.axis_size("tensor")
    column_start = tensor_index * feature_part
    normed_local = lax.dynamic_slice_in_dim(normed, column_start, feature_part, 1)
    query_full = jnp.dot(normed, w_query, preferred_element_type=jnp.float32) + query_bias
    partial_kv = jnp.dot(normed_local, w_keyvalue, preferred_element_type=jnp.float32)
    keyvalue = lax.psum(partial_kv, "tensor") + keyvalue_bias
    local_heads = w_query.shape[1] // HEAD_DIM
    kv_width = KV_HEADS * HEAD_DIM
    half_dim = HEAD_DIM // 2
    score_scale = HEAD_DIM ** (-0.5)
    group_index = tensor_index * local_heads // (HEADS // KV_HEADS)
    key_start = group_index * HEAD_DIM
    cosine, sine_table = tables(offset, HEAD_DIM)
    query_rot = rotate(
        query_full.reshape(row_count, local_heads, HEAD_DIM), cosine, sine_table
    ).astype(jnp.bfloat16)
    key_rot = rotate(
        lax.dynamic_slice_in_dim(keyvalue, key_start, HEAD_DIM, 1), cosine[:, 0], sine_table[:, 0]
    ).astype(jnp.bfloat16)
    value_one = lax.dynamic_slice_in_dim(keyvalue, kv_width + key_start, HEAD_DIM, 1).astype(
        jnp.bfloat16
    )
    places = jnp.arange(row_count, dtype=jnp.int32)
    allowed = (segment[:, None] == segment[None, :]) & (places[None, :] <= places[:, None])
    scores = (
        jnp.einsum("qhd,kd->hqk", query_rot, key_rot, preferred_element_type=jnp.float32)
        * score_scale
    )
    attn_weights = masked_softmax(scores, allowed[None])
    low_weights = attn_weights.astype(jnp.bfloat16)
    attended = jnp.einsum(
        "hqk,kd->qhd", low_weights, value_one, preferred_element_type=jnp.float32
    ).astype(jnp.bfloat16)
    upstream = grad_attention.reshape(row_count, local_heads, HEAD_DIM)
    weight_grad = jnp.einsum("qhd,kd->hqk", upstream, value_one, preferred_element_type=jnp.float32)
    value_grad = jnp.einsum(
        "hqk,qhd->kd", low_weights, upstream, preferred_element_type=jnp.float32
    )
    row_inner = jnp.sum(attn_weights * weight_grad, axis=-1, keepdims=True)
    score_grad = (attn_weights * (weight_grad - row_inner) * score_scale).astype(jnp.bfloat16)
    query_grad = unrotate(
        jnp.einsum("hqk,kd->qhd", score_grad, key_rot, preferred_element_type=jnp.float32),
        cosine,
        sine_table,
    ).astype(jnp.bfloat16)
    key_grad = jnp.einsum("hqk,qhd->kd", score_grad, query_rot, preferred_element_type=jnp.float32)
    zeros_kv = jnp.zeros((row_count, 2 * kv_width), jnp.float32)
    partial_grad = lax.dynamic_update_slice_in_dim(zeros_kv, key_grad, key_start, 1)
    partial_grad = lax.dynamic_update_slice_in_dim(
        partial_grad, value_grad, kv_width + key_start, 1
    )
    paired = (
        partial_grad.reshape(row_count, 2, KV_HEADS, 2, half_dim)
        .transpose(0, 1, 2, 4, 3)
        .reshape(row_count, 2 * kv_width)
    )
    share_width = 2 * kv_width // lane_count
    shared = lax.psum_scatter(paired, "tensor", scatter_dimension=1, tiled=True)
    position = tensor_index * share_width + jnp.arange(share_width // 2, dtype=jnp.int32) * 2
    frequency_index = position // 2 % half_dim
    is_key = (position < kv_width).astype(jnp.float32)
    frequency = ROPE_BASE ** (-2.0 * frequency_index.astype(jnp.float32) / HEAD_DIM)
    angles = offset.astype(jnp.float32)[:, None] * frequency[None, :]
    cos_pair = is_key[None, :] * jnp.cos(angles) + (1.0 - is_key[None, :])
    sin_pair = is_key[None, :] * jnp.sin(angles)
    pairs = shared.reshape(row_count, share_width // 2, 2)
    first_half = pairs[:, :, 0] * cos_pair + pairs[:, :, 1] * sin_pair
    second_half = pairs[:, :, 1] * cos_pair - pairs[:, :, 0] * sin_pair
    finished = (
        jnp.stack([first_half, second_half], axis=2)
        .reshape(row_count, share_width)
        .astype(jnp.bfloat16)
    )
    gathered = lax.all_gather(finished, "tensor", axis=1, tiled=True)
    kv_grad = (
        gathered.reshape(row_count, 2, KV_HEADS, half_dim, 2)
        .transpose(0, 1, 2, 4, 3)
        .reshape(row_count, 2 * kv_width)
    )
    query_flat = query_grad.reshape(row_count, local_heads * HEAD_DIM)
    query_part = contract_last(query_flat, w_query)
    normed_grad = lax.psum_scatter(
        query_part.astype(jnp.bfloat16), "tensor", scatter_dimension=1, tiled=True
    ).astype(jnp.float32) + contract_last(kv_grad, w_keyvalue)
    gain_local = lax.dynamic_slice_in_dim(norm_gain, column_start, feature_part, 0)
    hidden_local = local_rows.astype(jnp.float32)
    scaled = gain_local * normed_grad
    row_stat = lax.psum(jnp.sum(scaled * hidden_local, axis=1), "tensor") / D
    input_grad = (
        inverse[:, None] * scaled - hidden_local * (inverse**3 * row_stat)[:, None]
    ).astype(jnp.bfloat16)
    return (attended.reshape(row_count, local_heads * HEAD_DIM), input_grad)


VMEM, HBM = pltpu.VMEM, pltpu.HBM
CHUNKS = 1
EXTRA = 16


def call(kernel, out, ins, scratch=(), flops=0, moved=0, need=8):
    return pl.pallas_call(
        kernel,
        out_shape=[pltpu.VMEM(*item) if type(item) is tuple else item for item in out],
        in_specs=[pl.BlockSpec(memory_space=space) for _, space in ins],
        out_specs=[pl.BlockSpec(memory_space=VMEM) for _ in out],
        scratch_shapes=list(scratch),
        compiler_params=pltpu.CompilerParams(vmem_limit_bytes=need * 1024 * 1024),
        cost_estimate=pl.CostEstimate(flops=flops, bytes_accessed=moved, transcendentals=0),
    )(*[pltpu.with_memory_space_constraint(array, space) for array, space in ins])


def places():
    lane = lax.axis_index("tensor")
    near = jnp.where(lane & 1 == 1, 4, 2)
    far = 6 - near
    return [lane, lane ^ 1, lane ^ near, lane ^ (near + 1), lane ^ (far + 1), lane ^ far, lane ^ 6, lane ^ 7]


OWN, MATE, A0, A1, B0, B1, C0, C1 = range(8)
PAIRS = ((OWN, MATE), (A0, B0), (A1, B1), (C0, C1))


def pick_kernel(owner_in, slots_in, *refs):
    outs, (owner_ref, slots_ref, sems) = refs[:-3], refs[-3:]
    reads = [
        pltpu.make_async_copy(owner_in, owner_ref, sems.at[0]),
        pltpu.make_async_copy(slots_in, slots_ref, sems.at[1]),
    ]
    for read in reads:
        read.start()
    for read in reads:
        read.wait()
    count, me = owner_ref.shape[0], lax.axis_index("dp")
    part = slots_ref.shape[2] // CHUNKS
    for shift in range(count):
        target = lax.rem(me + shift, count)
        slot = jnp.int32(0)
        for j in range(owner_ref.shape[1]):
            slot = jnp.where(owner_ref[target, j] == me, j, slot)
        for chunk in range(CHUNKS):
            outs[shift * CHUNKS + chunk][...] = slots_ref[slot, :, chunk * part : (chunk + 1) * part]


def prepare_kernel(
    window,
    length_in,
    owner_in,
    frequency_ref,
    kv_in,
    gain_in,
    bias_in,
    kv_bias_in,
    upstream_in,
    w_in,
    kv_ref,
    gain_ref,
    bias_ref,
    kv_bias_ref,
    upstream_ref,
    chosen_ref,
    cos_ref,
    sin_ref,
    mask_ref,
    *refs,
):
    w_refs, (length_ref, owner_ref, sems) = refs[:-3], refs[-3:]
    reads = [
        pltpu.make_async_copy(length_in, length_ref, sems.at[0]),
        pltpu.make_async_copy(owner_in, owner_ref, sems.at[1]),
    ]
    pairs = (
        (kv_in, kv_ref),
        (gain_in, gain_ref),
        (bias_in, bias_ref),
        (kv_bias_in, kv_bias_ref),
        (upstream_in, upstream_ref),
    )
    depth = w_refs[0].shape[0]
    pairs += tuple(
        (w_in.at[pl.ds(pl.multiple_of(block * depth, depth), depth)], w_ref)
        for block, w_ref in zip(places(), w_refs)
    )
    copies = [pltpu.make_async_copy(a, b, sems.at[2 + i]) for i, (a, b) in enumerate(pairs)]
    for read in reads + copies:
        read.start()
    for read in reads:
        read.wait()
    count, me = length_ref.shape[0], lax.axis_index("dp")
    rows = cos_ref.shape[0]
    place = lax.broadcasted_iota(jnp.int32, (rows, window), 0)
    inside = lax.broadcasted_iota(jnp.int32, (rows, window), 1)
    row = lax.broadcasted_iota(jnp.int32, (rows, rows), 0)
    column = lax.broadcasted_iota(jnp.int32, (rows, rows), 1)
    row_segment = jnp.zeros((rows, rows), jnp.int32)
    column_segment = jnp.zeros((rows, rows), jnp.int32)
    position = lax.broadcasted_iota(jnp.int32, (rows, HEAD_DIM), 0)
    turn = position
    begin = jnp.int32(0)
    starts, sizes = [jnp.int32(0)] * count, [jnp.int32(0)] * count
    for j in range(count):
        size = length_ref[me, j]
        shift = lax.rem(me - owner_ref[me, j] + count, count)
        for k in range(count):
            starts[k] = jnp.where(shift == k, begin, starts[k])
            sizes[k] = jnp.where(shift == k, size, sizes[k])
        if j:
            row_segment += jnp.where(row >= begin, 1, 0)
            column_segment += jnp.where(column >= begin, 1, 0)
            turn = jnp.where(position >= begin, position - begin, turn)
        begin = begin + size
    for k in range(count):
        chosen = ((place - starts[k]) == inside) & (inside < sizes[k])
        chosen_ref[k] = jnp.where(chosen, 1.0, 0.0).astype(jnp.bfloat16)
    allowed = (row_segment == column_segment) & (column <= row)
    mask_ref[...] = jnp.where(allowed, 0.0, -1e30)
    angle = turn.astype(jnp.float32) * frequency_ref[...]
    low_half = lax.broadcasted_iota(jnp.int32, (rows, HEAD_DIM), 1) < HEAD_DIM // 2
    cos_ref[...] = jnp.cos(angle)
    sine = jnp.sin(angle)
    sin_ref[...] = jnp.where(low_half, -sine, sine)
    for copy in copies:
        copy.wait()


def pack_kernel(chosen_ref, *refs):
    windows, out_ref = refs[:-1], refs[-1]
    total = jnp.zeros(out_ref.shape, jnp.float32)
    for k in range(len(windows)):
        total += jnp.dot(chosen_ref[k], windows[k][...], preferred_element_type=jnp.float32)
    out_ref[...] = total.astype(jnp.bfloat16)


def keyvalue_kernel(*refs):
    pieces, (gain_ref, w_ref, keep_ref, send_ref, products) = refs[:-5], refs[-5:]
    me = lax.axis_index("tensor")
    part = pieces[0].shape[1]
    gain = gain_ref[me]
    scaled = [
        (piece[...].astype(jnp.float32) * gain[:, i * part : (i + 1) * part]).astype(jnp.bfloat16)
        for i, piece in enumerate(pieces)
    ]
    heads = products.shape[0]
    step = 4 * HEAD_DIM
    for start in range(0, w_ref.shape[1], step):
        product = sum(
            jnp.dot(
                scaled[i],
                w_ref[i * part : (i + 1) * part, start : start + step],
                preferred_element_type=jnp.float32,
            )
            for i in range(len(pieces))
        ).astype(jnp.bfloat16)
        for k in range(step // HEAD_DIM):
            column = start // HEAD_DIM + k
            lanes = slice(column // heads * HEAD_DIM, (column // heads + 1) * HEAD_DIM)
            products[column % heads, :, lanes] = product[:, k * HEAD_DIM : (k + 1) * HEAD_DIM]
    for chip in range(heads // 2):
        keep_ref[chip] = products[me ^ (2 * chip)]
        send_ref[chip] = products[me ^ (2 * chip + 1)]


def chip_sum_kernel(keep_ref, other_ref, *outs):
    for chip, out in enumerate(outs):
        out[...] = (
            keep_ref[chip].astype(jnp.float32) + other_ref[chip].astype(jnp.float32)
        ).astype(jnp.bfloat16)


def query_kernel(names, chunk, first, *refs):
    pieces, refs = refs[: len(names)], refs[len(names) :]
    w_refs, gain_ref, refs = refs[: len(names)], refs[len(names)], refs[len(names) + 1 :]
    acc_ref, square_ref = refs[-2:]
    part = pieces[0].shape[1]
    at = places()
    squares = jnp.zeros(square_ref.shape, jnp.float32) if first else refs[1][...]
    for i, name in enumerate(names):
        wide = pieces[i][...].astype(jnp.float32)
        square = wide * wide
        for k in range(part // HEAD_DIM):
            squares += square[:, k * HEAD_DIM : (k + 1) * HEAD_DIM]
        scaled = (wide * gain_ref[at[name], :, chunk * part : (chunk + 1) * part]).astype(jnp.bfloat16)
        w_part = w_refs[i][chunk * part : (chunk + 1) * part, :]
        product = jnp.dot(scaled, w_part, preferred_element_type=jnp.float32)
        if i == 0 and not first:
            acc_ref[...] = refs[0][...] + product
        elif i == 0:
            acc_ref[...] = product
        else:
            acc_ref[...] += product
    square_ref[...] = squares


def dot_nt(left, right):
    return lax.dot_general(left, right, (((1,), (1,)), ((), ())), preferred_element_type=jnp.float32)


def dot_tn(left, right):
    return lax.dot_general(left, right, (((0,), (0,)), ((), ())), preferred_element_type=jnp.float32)


def attention_kernel(
    width,
    acc_ref,
    square_ref,
    own_kv,
    x_kv,
    y_kv,
    d_kv,
    cos_ref,
    sin_ref,
    mask_ref,
    bias_ref,
    kv_bias_ref,
    upstream_ref,
    attended_ref,
    query_grad_ref,
    kv_grad_ref,
    inverse_ref,
):
    rows = acc_ref.shape[0]
    heads = acc_ref.shape[1] // HEAD_DIM
    block = lax.axis_index("tensor")
    scale = HEAD_DIM ** (-0.5)
    inverse = lax.rsqrt(jnp.sum(square_ref[...], axis=1, keepdims=True) / width + EPSILON)
    cosine, sine = cos_ref[...], sin_ref[...]

    def rot(u):
        return u * cosine + pltpu.roll(u, HEAD_DIM // 2, 1) * sine

    def unrot(z):
        return z * cosine - pltpu.roll(z, HEAD_DIM // 2, 1) * sine

    kv_acc = sum(part[...].astype(jnp.float32) for part in (own_kv, x_kv, y_kv, d_kv))
    key_acc, value_acc = kv_acc[:, :HEAD_DIM], kv_acc[:, HEAD_DIM:]
    key = rot(key_acc * inverse + kv_bias_ref[block]).astype(jnp.bfloat16)
    value = (value_acc * inverse + kv_bias_ref[KV_HEADS + block]).astype(jnp.bfloat16)
    parts = [slice(h * HEAD_DIM, (h + 1) * HEAD_DIM) for h in range(heads)]
    bands = [slice(h * rows, (h + 1) * rows) for h in range(heads)]
    accs = [acc_ref[:, part] for part in parts]
    queries = [
        rot(acc * inverse + bias_ref[:, part]).astype(jnp.bfloat16) for acc, part in zip(accs, parts)
    ]
    upstreams = [upstream_ref[:, part] for part in parts]
    all_scores = dot_nt(jnp.concatenate(queries, axis=0), key)
    all_weight_grads = dot_nt(jnp.concatenate(upstreams, axis=0), value)
    scores = [all_scores[band] * scale + mask_ref[...] for band in bands]
    weight_grads = [all_weight_grads[band] for band in bands]
    highest = [jnp.max(score, axis=1, keepdims=True) for score in scores]
    exponents = [jnp.exp(score - high) for score, high in zip(scores, highest)]
    scales = [1.0 / jnp.sum(exponent, axis=1, keepdims=True) for exponent in exponents]
    weights = [exponent * one for exponent, one in zip(exponents, scales)]
    row_inners = [
        jnp.sum(weight * grad, axis=1, keepdims=True) for weight, grad in zip(weights, weight_grads)
    ]
    lows = [weight.astype(jnp.bfloat16) for weight in weights]
    score_grads = [
        (weight * (grad - row_inner)).astype(jnp.bfloat16)
        for weight, grad, row_inner in zip(weights, weight_grads, row_inners)
    ]
    attended = [jnp.dot(low, value, preferred_element_type=jnp.float32) for low in lows]
    turned = [jnp.dot(grad, key, preferred_element_type=jnp.float32) * scale for grad in score_grads]
    inner = jnp.zeros((rows, HEAD_DIM), jnp.float32)
    key_sum = jnp.zeros((HEAD_DIM, rows), jnp.float32)
    value_sum = jnp.zeros((HEAD_DIM, rows), jnp.float32)
    for h, part in enumerate(parts):
        attended_ref[:, part] = attended[h].astype(jnp.bfloat16)
        query_grad = unrot(turned[h]).astype(jnp.bfloat16)
        query_grad_ref[:, part] = query_grad
        inner += query_grad.astype(jnp.float32) * accs[h]
        key_sum += dot_tn(queries[h], score_grads[h])
        value_sum += dot_tn(upstreams[h], lows[h])
    key_grad, value_grad = key_sum.T * scale, value_sum.T
    key_low, value_low = unrot(key_grad).astype(jnp.bfloat16), value_grad.astype(jnp.bfloat16)
    inner += key_low.astype(jnp.float32) * key_acc + value_low.astype(jnp.float32) * value_acc
    kv_grad_ref[:rows, :HEAD_DIM] = key_low
    kv_grad_ref[:rows, HEAD_DIM:] = value_low
    row = lax.broadcasted_iota(jnp.int32, (rows, 2 * HEAD_DIM), 0)
    column = lax.broadcasted_iota(jnp.int32, (rows, 2 * HEAD_DIM), 1)
    column_sum = jnp.sum(inner, axis=1, keepdims=True)
    as_row = jnp.sum(jnp.where(row == column, column_sum, 0.0), axis=0, keepdims=True)
    high = as_row.astype(jnp.bfloat16).astype(jnp.float32)
    middle = (as_row - high).astype(jnp.bfloat16).astype(jnp.float32)
    last = as_row - high - middle
    index = lax.broadcasted_iota(jnp.int32, (EXTRA, 2 * HEAD_DIM), 0)
    tail = jnp.where(index == 0, high, 0.0)
    tail = jnp.where(index == 1, middle, tail)
    tail = jnp.where(index == 2, last, tail)
    kv_grad_ref[rows:, :] = tail.astype(jnp.bfloat16)
    inverse_ref[...] = jnp.broadcast_to(inverse, inverse_ref.shape)


def gradient_kernel(grad_ref, w_ref, *refs):
    added, out_ref = refs[:-1], refs[-1]
    total = dot_nt(grad_ref[...], w_ref[...])
    for more in added:
        total += more[...].astype(jnp.float32)
    out_ref[...] = total.astype(out_ref.dtype)


def add_kernel(left_ref, right_ref, out_ref):
    out_ref[...] = (left_ref[...] + right_ref[...].astype(jnp.float32)).astype(out_ref.dtype)


def keyvalue_gradient_kernel(*refs):
    pieces, (before_ref, w_ref, out_ref, inner_ref, joined) = refs[:-5], refs[-5:]
    rows = out_ref.shape[0]
    half = len(pieces) * HEAD_DIM
    at = places()
    tail = jnp.zeros((EXTRA, 2 * HEAD_DIM), jnp.float32)
    for i, piece in enumerate(pieces):
        for part in range(2):
            start = pl.multiple_of(part * half + at[i] * HEAD_DIM, HEAD_DIM)
            joined[:, pl.ds(start, HEAD_DIM)] = piece[:rows, part * HEAD_DIM : (part + 1) * HEAD_DIM]
        tail += piece[rows:, :].astype(jnp.float32)
    out_ref[...] = before_ref[...] + dot_nt(joined[...], w_ref[...])
    as_row = jnp.sum(tail, axis=0, keepdims=True)
    row = lax.broadcasted_iota(jnp.int32, (rows, 2 * HEAD_DIM), 0)
    column = lax.broadcasted_iota(jnp.int32, (rows, 2 * HEAD_DIM), 1)
    as_column = jnp.sum(jnp.where(row == column, as_row, 0.0), axis=1, keepdims=True)
    inner_ref[...] = jnp.broadcast_to(as_column, inner_ref.shape)


def finish_kernel(width, sum_ref, mate_ref, last_ref, inner_ref, inverse_ref, gain_ref, *refs):
    pieces, out_ref = refs[:-1], refs[-1]
    part = pieces[0].shape[1]
    inverse = inverse_ref[:, :1]
    factor = inverse * inverse * inverse * (inner_ref[:, :1] / width)
    gain = gain_ref[lax.axis_index("tensor")]
    for i, piece in enumerate(pieces):
        lanes = slice(i * part, (i + 1) * part)
        normed_grad = sum_ref[:, lanes] + mate_ref[:, lanes].astype(jnp.float32)
        normed_grad += last_ref[:, lanes].astype(jnp.float32)
        out_ref[:, lanes] = (
            inverse * (gain[:, lanes] * normed_grad) - piece[...].astype(jnp.float32) * factor
        ).astype(jnp.bfloat16)


def cube_device(
    hidden_slots,
    lengths,
    owners,
    norm_gain,
    w_query,
    query_bias,
    w_keyvalue,
    keyvalue_bias,
    grad_attention,
):
    window, depth = hidden_slots.shape[1:]
    owner_count, lane_count = lax.axis_size("dp"), lax.axis_size("tensor")
    rows, columns = grad_attention.shape
    width, part = depth * lane_count, depth // CHUNKS
    half, full = jnp.bfloat16, jnp.float32

    def permute(value, partner):
        return lax.ppermute(value, "tensor", [(i, partner(i)) for i in range(lane_count)])

    def swap(value):
        return permute(value, lambda i: i ^ 1)

    def near(value):
        return permute(value, lambda i: i ^ (4 if i & 1 else 2))

    def far(value):
        return permute(value, lambda i: i ^ (2 if i & 1 else 4))

    windows = call(
        pick_kernel,
        [((window, part), half)] * (owner_count * CHUNKS),
        [(owners, HBM), (hidden_slots, HBM)],
        scratch=[
            pltpu.SMEM(owners.shape, jnp.int32),
            pltpu.VMEM(hidden_slots.shape, half),
            pltpu.SemaphoreType.DMA((2,)),
        ],
        moved=4 * hidden_slots.size,
    )
    arrived = [[windows[chunk]] for chunk in range(CHUNKS)]
    for chunk in range(CHUNKS):
        for shift in range(1, owner_count):
            pairs = [(i, (i + shift) % owner_count) for i in range(owner_count)]
            arrived[chunk].append(lax.ppermute(windows[shift * CHUNKS + chunk], "dp", pairs))
    frequency = ROPE_BASE ** (-2.0 * jnp.arange(HEAD_DIM // 2, dtype=full) / HEAD_DIM)
    frequency = jnp.concatenate([frequency, frequency])[None]
    w_kv, gain, bias, kv_bias, upstream, chosen, cosine, sine, mask, *w = call(
        functools.partial(prepare_kernel, window),
        [
            (w_keyvalue.shape, half),
            ((lane_count, 1, depth), full),
            ((1, columns), full),
            ((2 * KV_HEADS, 1, HEAD_DIM), full),
            (grad_attention.shape, half),
            ((owner_count, rows, window), half),
            ((rows, HEAD_DIM), full),
            ((rows, HEAD_DIM), full),
            ((rows, rows), full),
        ]
        + [((depth, columns), half)] * lane_count,
        [
            (lengths, HBM),
            (owners, HBM),
            (frequency, VMEM),
            (w_keyvalue, HBM),
            (norm_gain.reshape(lane_count, 1, depth), HBM),
            (query_bias.reshape(1, columns), HBM),
            (keyvalue_bias.reshape(2 * KV_HEADS, 1, HEAD_DIM), HBM),
            (grad_attention, HBM),
            (w_query, HBM),
        ],
        scratch=[
            pltpu.SMEM(lengths.shape, jnp.int32),
            pltpu.SMEM(owners.shape, jnp.int32),
            pltpu.SemaphoreType.DMA((7 + lane_count,)),
        ],
        flops=64 * rows * rows,
        moved=2 * w_query.size,
        need=32,
    )
    sums = None

    def query(chunk, names, pieces):
        nonlocal sums
        sums = call(
            functools.partial(query_kernel, names, chunk, sums is None),
            [((rows, columns), full), ((rows, HEAD_DIM), full)],
            [(piece, VMEM) for piece in pieces]
            + [(w[name], VMEM) for name in names]
            + [(gain, VMEM)]
            + [(value, VMEM) for value in sums or ()],
            flops=2 * rows * part * columns * len(names),
            moved=len(names) * part * columns * 2,
        )

    local, groups = [], []
    for chunk in range(CHUNKS):
        (own,) = call(
            pack_kernel,
            [((rows, part), half)],
            [(chosen, VMEM)] + [(piece, VMEM) for piece in arrived[chunk]],
            flops=2 * rows * window * owner_count * part,
            moved=4 * rows * part * 2,
        )
        local.append(own)
        a0 = near(own)
        mate = swap(own)
        a1 = near(mate)
        b0 = swap(a0)
        c0 = far(a0)
        b1 = swap(a1)
        c1 = swap(c0)
        groups.append([own, mate, a0, a1, b0, b1, c0, c1])
    for chunk in range(CHUNKS):
        group = groups[chunk]
        for names in PAIRS:
            query(chunk, names, [group[n] for n in names])
    acc, square = sums

    kv_shape = (lane_count // 2, rows, 2 * HEAD_DIM)
    keep, send = call(
        keyvalue_kernel,
        [(kv_shape, half), (kv_shape, half)],
        [(piece, VMEM) for piece in local] + [(gain, VMEM), (w_kv, VMEM)],
        scratch=[pltpu.VMEM((lane_count, rows, 2 * HEAD_DIM), half)],
        flops=2 * rows * depth * w_keyvalue.shape[1],
        moved=w_keyvalue.size * 2,
        need=16,
    )
    other = swap(send)
    kv_parts = call(
        chip_sum_kernel,
        [(kv_shape[1:], half)] * (lane_count // 2),
        [(keep, VMEM), (other, VMEM)],
        flops=rows * depth,
        moved=rows * depth * 6,
    )
    kv_parts = [kv_parts[0]] + [
        permute(kv_parts[chip], lambda i, chip=chip: i ^ (2 * chip))
        for chip in range(1, lane_count // 2)
    ]

    attended, query_grad, kv_grad, inverse = call(
        functools.partial(attention_kernel, width),
        [
            ((rows, columns), half),
            ((rows, columns), half),
            ((rows + EXTRA, 2 * HEAD_DIM), half),
            ((rows, HEAD_DIM), full),
        ],
        [(acc, VMEM), (square, VMEM)]
        + [(piece, VMEM) for piece in kv_parts]
        + [(value, VMEM) for value in (cosine, sine, mask, bias, kv_bias, upstream)],
        flops=14 * rows * rows * columns,
        moved=rows * columns * 10,
        need=32,
    )

    def gradient(name, added=(), kind=half):
        return call(
            gradient_kernel,
            [((rows, depth), kind)],
            [(query_grad, VMEM), (w[name], VMEM)] + [(value, VMEM) for value in added],
            flops=2 * rows * depth * columns,
            moved=depth * columns * 2,
        )

    (to_c1,) = gradient(C1)
    from_c1 = swap(to_c1)
    (to_b1,) = gradient(B1)
    from_b1 = swap(to_b1)
    (to_c0,) = gradient(C0, (from_c1,))
    from_far = far(to_c0)
    (to_a1,) = gradient(A1, (from_b1,))
    near_mate = near(to_a1)
    (to_b0,) = gradient(B0)
    from_b0 = swap(to_b0)

    kv_mate, kv_a0 = swap(kv_grad), near(kv_grad)
    kv_a1 = near(kv_mate)
    kv_b0, kv_c0 = swap(kv_a0), far(kv_a0)
    kv_b1, kv_c1 = swap(kv_a1), swap(kv_c0)

    (part_a0,) = gradient(A0, (from_b0,), full)
    (to_a0,) = call(
        add_kernel,
        [((rows, depth), half)],
        [(part_a0, VMEM), (from_far, VMEM)],
        flops=rows * depth,
        moved=rows * depth * 8,
    )
    near_own = near(to_a0)
    (to_own,) = gradient(OWN, (), full)
    (to_mate,) = gradient(MATE, (near_mate,))
    from_mate = swap(to_mate)
    total, inner = call(
        keyvalue_gradient_kernel,
        [((rows, depth), full), ((rows, HEAD_DIM), full)],
        [(piece, VMEM) for piece in (kv_grad, kv_mate, kv_a0, kv_a1, kv_b0, kv_b1, kv_c0, kv_c1)]
        + [(to_own, VMEM), (w_kv, VMEM)],
        scratch=[pltpu.VMEM((rows, w_keyvalue.shape[1]), half)],
        flops=2 * rows * depth * w_keyvalue.shape[1],
        moved=w_keyvalue.size * 2,
        need=16,
    )
    (input_grad,) = call(
        functools.partial(finish_kernel, width),
        [jax.ShapeDtypeStruct((rows, depth), half)],
        [(value, VMEM) for value in (total, from_mate, near_own, inner, inverse, gain)]
        + [(piece, VMEM) for piece in local],
        flops=8 * rows * depth,
        moved=rows * depth * 14,
    )
    return attended, input_grad


def solution(mesh):
    in_specs = (
        P("dp", None, "tensor"),
        P(),
        P(),
        P(),
        P(None, "tensor"),
        P("tensor"),
        P("tensor", None),
        P(),
        P("dp", "tensor"),
    )
    out_specs = (P("dp", "tensor"), P("dp", "tensor"))
    cube = mesh.shape["tensor"] == 8 and KV_HEADS == 8

    def layer(*args):
        return cube_device(*args)

    return jax.shard_map(
        layer if cube else on_device,
        mesh=mesh,
        in_specs=in_specs,
        out_specs=out_specs,
        check_vma=False,
    )
```

```python
import functools

import jax
import jax.numpy as jnp
from jax import lax
from jax.experimental import pallas as pl
from jax.experimental.pallas import tpu as pltpu
from jax.sharding import PartitionSpec as P

D = 8192
HEADS = 64
KV_HEADS = 8
HEAD_DIM = 128


EPSILON = 1e-06
ROPE_BASE = 1000000.0


def packing(length_row, row_count):
    starts = jnp.cumsum(length_row) - length_row
    places = jnp.arange(row_count, dtype=jnp.int32)
    segment = jnp.sum((places[:, None] >= starts[None, 1:]).astype(jnp.int32), axis=1)
    onehot = (segment[:, None] == jnp.arange(length_row.shape[0], dtype=jnp.int32)[None, :]).astype(
        jnp.int32
    )
    offset = places - jnp.sum(onehot * starts[None, :], axis=1)
    return (segment, offset, onehot)


def tables(offset, head_width):
    halfway = head_width // 2
    frequency = ROPE_BASE ** (-2.0 * jnp.arange(halfway, dtype=jnp.float32) / head_width)
    angles = offset.astype(jnp.float32)[:, None] * frequency[None, :]
    angles = jnp.concatenate([angles, angles], axis=1)
    return (jnp.cos(angles)[:, None, :], jnp.sin(angles)[:, None, :])


def rotate(values, cosine, sine_table):
    halfway = values.shape[-1] // 2
    turned = jnp.concatenate([-values[..., halfway:], values[..., :halfway]], axis=-1)
    return values * cosine + turned * sine_table


def unrotate(gradient, cosine, sine_table):
    halfway = gradient.shape[-1] // 2
    scaled = gradient * sine_table
    turned = jnp.concatenate([scaled[..., halfway:], -scaled[..., :halfway]], axis=-1)
    return gradient * cosine + turned


def normalize(hidden, norm_gain):
    widened = hidden.astype(jnp.float32)
    inverse = lax.rsqrt(jnp.mean(widened * widened, axis=1) + EPSILON)
    normed = (widened * inverse[:, None] * norm_gain).astype(jnp.bfloat16)
    return (widened, inverse, normed)


def masked_softmax(scores, allowed):
    scores = jnp.where(allowed, scores, -1e30)
    highest = jnp.max(scores, axis=-1, keepdims=True)
    exponent = jnp.where(allowed, jnp.exp(scores - highest), 0.0)
    return exponent / jnp.sum(exponent, axis=-1, keepdims=True)


def contract_last(operand, weights):
    return lax.dot_general(
        operand, weights, (((1,), (1,)), ((), ())), preferred_element_type=jnp.float32
    )


def on_device(
    hidden_slots,
    lengths,
    owners,
    norm_gain,
    w_query,
    query_bias,
    w_keyvalue,
    keyvalue_bias,
    grad_attention,
):
    _, window, feature_part = hidden_slots.shape
    owner_count = lax.axis_size("dp")
    dp_index = lax.axis_index("dp")
    picked = (owners == dp_index).astype(jnp.bfloat16)
    outgoing = jnp.einsum(
        "bj,jld->bld", picked, hidden_slots, preferred_element_type=jnp.float32
    ).astype(jnp.bfloat16)
    arrived = lax.all_to_all(outgoing, "dp", split_axis=0, concat_axis=0, tiled=True)
    row_count = grad_attention.shape[0]
    length_row = lax.dynamic_index_in_dim(lengths, dp_index, 0, keepdims=False)
    owner_row = lax.dynamic_index_in_dim(owners, dp_index, 0, keepdims=False)
    segment, offset, onehot = packing(length_row, row_count)
    source = jnp.sum(onehot * owner_row[None, :], axis=1)
    row_index = source * window + offset
    local_rows = jnp.take(arrived.reshape(owner_count * window, feature_part), row_index, axis=0)
    full_rows = lax.all_gather(local_rows, "tensor", axis=1, tiled=True)
    _, inverse, normed = normalize(full_rows, norm_gain)
    tensor_index = lax.axis_index("tensor")
    lane_count = lax.axis_size("tensor")
    column_start = tensor_index * feature_part
    normed_local = lax.dynamic_slice_in_dim(normed, column_start, feature_part, 1)
    query_full = jnp.dot(normed, w_query, preferred_element_type=jnp.float32) + query_bias
    partial_kv = jnp.dot(normed_local, w_keyvalue, preferred_element_type=jnp.float32)
    keyvalue = lax.psum(partial_kv, "tensor") + keyvalue_bias
    local_heads = w_query.shape[1] // HEAD_DIM
    kv_width = KV_HEADS * HEAD_DIM
    half_dim = HEAD_DIM // 2
    score_scale = HEAD_DIM ** (-0.5)
    group_index = tensor_index * local_heads // (HEADS // KV_HEADS)
    key_start = group_index * HEAD_DIM
    cosine, sine_table = tables(offset, HEAD_DIM)
    query_rot = rotate(
        query_full.reshape(row_count, local_heads, HEAD_DIM), cosine, sine_table
    ).astype(jnp.bfloat16)
    key_rot = rotate(
        lax.dynamic_slice_in_dim(keyvalue, key_start, HEAD_DIM, 1), cosine[:, 0], sine_table[:, 0]
    ).astype(jnp.bfloat16)
    value_one = lax.dynamic_slice_in_dim(keyvalue, kv_width + key_start, HEAD_DIM, 1).astype(
        jnp.bfloat16
    )
    places = jnp.arange(row_count, dtype=jnp.int32)
    allowed = (segment[:, None] == segment[None, :]) & (places[None, :] <= places[:, None])
    scores = (
        jnp.einsum("qhd,kd->hqk", query_rot, key_rot, preferred_element_type=jnp.float32)
        * score_scale
    )
    attn_weights = masked_softmax(scores, allowed[None])
    low_weights = attn_weights.astype(jnp.bfloat16)
    attended = jnp.einsum(
        "hqk,kd->qhd", low_weights, value_one, preferred_element_type=jnp.float32
    ).astype(jnp.bfloat16)
    upstream = grad_attention.reshape(row_count, local_heads, HEAD_DIM)
    weight_grad = jnp.einsum("qhd,kd->hqk", upstream, value_one, preferred_element_type=jnp.float32)
    value_grad = jnp.einsum(
        "hqk,qhd->kd", low_weights, upstream, preferred_element_type=jnp.float32
    )
    row_inner = jnp.sum(attn_weights * weight_grad, axis=-1, keepdims=True)
    score_grad = (attn_weights * (weight_grad - row_inner) * score_scale).astype(jnp.bfloat16)
    query_grad = unrotate(
        jnp.einsum("hqk,kd->qhd", score_grad, key_rot, preferred_element_type=jnp.float32),
        cosine,
        sine_table,
    ).astype(jnp.bfloat16)
    key_grad = jnp.einsum("hqk,qhd->kd", score_grad, query_rot, preferred_element_type=jnp.float32)
    zeros_kv = jnp.zeros((row_count, 2 * kv_width), jnp.float32)
    partial_grad = lax.dynamic_update_slice_in_dim(zeros_kv, key_grad, key_start, 1)
    partial_grad = lax.dynamic_update_slice_in_dim(
        partial_grad, value_grad, kv_width + key_start, 1
    )
    paired = (
        partial_grad.reshape(row_count, 2, KV_HEADS, 2, half_dim)
        .transpose(0, 1, 2, 4, 3)
        .reshape(row_count, 2 * kv_width)
    )
    share_width = 2 * kv_width // lane_count
    shared = lax.psum_scatter(paired, "tensor", scatter_dimension=1, tiled=True)
    position = tensor_index * share_width + jnp.arange(share_width // 2, dtype=jnp.int32) * 2
    frequency_index = position // 2 % half_dim
    is_key = (position < kv_width).astype(jnp.float32)
    frequency = ROPE_BASE ** (-2.0 * frequency_index.astype(jnp.float32) / HEAD_DIM)
    angles = offset.astype(jnp.float32)[:, None] * frequency[None, :]
    cos_pair = is_key[None, :] * jnp.cos(angles) + (1.0 - is_key[None, :])
    sin_pair = is_key[None, :] * jnp.sin(angles)
    pairs = shared.reshape(row_count, share_width // 2, 2)
    first_half = pairs[:, :, 0] * cos_pair + pairs[:, :, 1] * sin_pair
    second_half = pairs[:, :, 1] * cos_pair - pairs[:, :, 0] * sin_pair
    finished = (
        jnp.stack([first_half, second_half], axis=2)
        .reshape(row_count, share_width)
        .astype(jnp.bfloat16)
    )
    gathered = lax.all_gather(finished, "tensor", axis=1, tiled=True)
    kv_grad = (
        gathered.reshape(row_count, 2, KV_HEADS, half_dim, 2)
        .transpose(0, 1, 2, 4, 3)
        .reshape(row_count, 2 * kv_width)
    )
    query_flat = query_grad.reshape(row_count, local_heads * HEAD_DIM)
    query_part = contract_last(query_flat, w_query)
    normed_grad = lax.psum_scatter(
        query_part.astype(jnp.bfloat16), "tensor", scatter_dimension=1, tiled=True
    ).astype(jnp.float32) + contract_last(kv_grad, w_keyvalue)
    gain_local = lax.dynamic_slice_in_dim(norm_gain, column_start, feature_part, 0)
    hidden_local = local_rows.astype(jnp.float32)
    scaled = gain_local * normed_grad
    row_stat = lax.psum(jnp.sum(scaled * hidden_local, axis=1), "tensor") / D
    input_grad = (
        inverse[:, None] * scaled - hidden_local * (inverse**3 * row_stat)[:, None]
    ).astype(jnp.bfloat16)
    return (attended.reshape(row_count, local_heads * HEAD_DIM), input_grad)


VMEM, HBM = pltpu.VMEM, pltpu.HBM
CHUNKS = 1
EXTRA = 8
BANDS = 4


def call(kernel, out, ins, scratch=(), flops=0, moved=0, need=8):
    return pl.pallas_call(
        kernel,
        out_shape=[pltpu.VMEM(*item) if type(item) is tuple else item for item in out],
        in_specs=[pl.BlockSpec(memory_space=space) for _, space in ins],
        out_specs=[
            pl.BlockSpec(memory_space=VMEM if type(item) is tuple else pl.ANY) for item in out
        ],
        scratch_shapes=list(scratch),
        compiler_params=pltpu.CompilerParams(vmem_limit_bytes=need * 1024 * 1024),
        cost_estimate=pl.CostEstimate(flops=flops, bytes_accessed=moved, transcendentals=0),
    )(*[pltpu.with_memory_space_constraint(array, space) for array, space in ins])


def places():
    lane = lax.axis_index("tensor")
    near = jnp.where(lane & 1 == 1, 4, 2)
    far = 6 - near
    return [lane, lane ^ 1, lane ^ near, lane ^ (near + 1), lane ^ (far + 1), lane ^ far, lane ^ 6, lane ^ 7]


OWN, MATE, A0, A1, B0, B1, C0, C1 = range(8)
GROUPS = ((OWN, MATE), (A0, B0), (A1, B1), (C0,), (C1,))


def pick_kernel(owner_in, slots_in, *refs):
    outs, (owner_ref, slots_ref, sems) = refs[:-3], refs[-3:]
    reads = [
        pltpu.make_async_copy(owner_in, owner_ref, sems.at[0]),
        pltpu.make_async_copy(slots_in, slots_ref, sems.at[1]),
    ]
    for read in reads:
        read.start()
    for read in reads:
        read.wait()
    count, me = owner_ref.shape[0], lax.axis_index("dp")
    part = slots_ref.shape[2] // CHUNKS
    for shift in range(count):
        target = lax.rem(me + shift, count)
        slot = jnp.int32(0)
        for j in range(owner_ref.shape[1]):
            slot = jnp.where(owner_ref[target, j] == me, j, slot)
        for chunk in range(CHUNKS):
            outs[shift * CHUNKS + chunk][...] = slots_ref[slot, :, chunk * part : (chunk + 1) * part]


def prepare_kernel(
    window,
    length_in,
    owner_in,
    frequency_ref,
    kv_in,
    gain_in,
    bias_in,
    kv_bias_in,
    upstream_in,
    w_in,
    kv_ref,
    gain_ref,
    bias_ref,
    kv_bias_ref,
    upstream_ref,
    chosen_ref,
    cos_ref,
    sin_ref,
    mask_ref,
    *refs,
):
    w_refs, (length_ref, owner_ref, sems) = refs[:-3], refs[-3:]
    reads = [
        pltpu.make_async_copy(length_in, length_ref, sems.at[0]),
        pltpu.make_async_copy(owner_in, owner_ref, sems.at[1]),
    ]
    pairs = (
        (kv_in, kv_ref),
        (gain_in, gain_ref),
        (bias_in, bias_ref),
        (kv_bias_in, kv_bias_ref),
        (upstream_in, upstream_ref),
    )
    depth = w_refs[0].shape[0]
    pairs += tuple(
        (w_in.at[pl.ds(pl.multiple_of(block * depth, depth), depth)], w_ref)
        for block, w_ref in zip(places(), w_refs)
    )
    copies = [pltpu.make_async_copy(a, b, sems.at[2 + i]) for i, (a, b) in enumerate(pairs)]
    for read in reads + copies:
        read.start()
    for read in reads:
        read.wait()
    count, me = length_ref.shape[0], lax.axis_index("dp")
    rows = cos_ref.shape[0]
    place = lax.broadcasted_iota(jnp.int32, (rows, window), 0)
    inside = lax.broadcasted_iota(jnp.int32, (rows, window), 1)
    row = lax.broadcasted_iota(jnp.int32, (rows, rows), 0)
    column = lax.broadcasted_iota(jnp.int32, (rows, rows), 1)
    row_segment = jnp.zeros((rows, rows), jnp.int32)
    column_segment = jnp.zeros((rows, rows), jnp.int32)
    position = lax.broadcasted_iota(jnp.int32, (rows, HEAD_DIM), 0)
    turn = position
    begin = jnp.int32(0)
    starts, sizes = [jnp.int32(0)] * count, [jnp.int32(0)] * count
    for j in range(count):
        size = length_ref[me, j]
        shift = lax.rem(me - owner_ref[me, j] + count, count)
        for k in range(count):
            starts[k] = jnp.where(shift == k, begin, starts[k])
            sizes[k] = jnp.where(shift == k, size, sizes[k])
        if j:
            row_segment += jnp.where(row >= begin, 1, 0)
            column_segment += jnp.where(column >= begin, 1, 0)
            turn = jnp.where(position >= begin, position - begin, turn)
        begin = begin + size
    for k in range(count):
        chosen = ((place - starts[k]) == inside) & (inside < sizes[k])
        chosen_ref[k] = jnp.where(chosen, 1.0, 0.0).astype(jnp.bfloat16)
    allowed = (row_segment == column_segment) & (column <= row)
    mask_ref[...] = jnp.where(allowed, 0.0, -1e30)
    angle = turn.astype(jnp.float32) * frequency_ref[...]
    low_half = lax.broadcasted_iota(jnp.int32, (rows, HEAD_DIM), 1) < HEAD_DIM // 2
    cos_ref[...] = jnp.cos(angle)
    sine = jnp.sin(angle)
    sin_ref[...] = jnp.where(low_half, -sine, sine)
    for copy in copies:
        copy.wait()


def pack_kernel(chosen_ref, *refs):
    windows, out_ref = refs[:-1], refs[-1]
    total = jnp.zeros(out_ref.shape, jnp.float32)
    for k in range(len(windows)):
        total += jnp.dot(chosen_ref[k], windows[k][...], preferred_element_type=jnp.float32)
    out_ref[...] = total.astype(jnp.bfloat16)


def keyvalue_kernel(*refs):
    pieces, (gain_ref, w_ref, keep_ref, send_ref, products) = refs[:-5], refs[-5:]
    me = lax.axis_index("tensor")
    part = pieces[0].shape[1]
    gain = gain_ref[me]
    scaled = [
        (piece[...].astype(jnp.float32) * gain[:, i * part : (i + 1) * part]).astype(jnp.bfloat16)
        for i, piece in enumerate(pieces)
    ]
    heads = products.shape[0]
    step = 4 * HEAD_DIM
    for start in range(0, w_ref.shape[1], step):
        product = sum(
            jnp.dot(
                scaled[i],
                w_ref[i * part : (i + 1) * part, start : start + step],
                preferred_element_type=jnp.float32,
            )
            for i in range(len(pieces))
        ).astype(jnp.bfloat16)
        for k in range(step // HEAD_DIM):
            column = start // HEAD_DIM + k
            lanes = slice(column // heads * HEAD_DIM, (column // heads + 1) * HEAD_DIM)
            products[column % heads, :, lanes] = product[:, k * HEAD_DIM : (k + 1) * HEAD_DIM]
    for chip in range(heads // 2):
        keep_ref[chip] = products[me ^ (2 * chip)]
        send_ref[chip] = products[me ^ (2 * chip + 1)]


def chip_sum_kernel(keep_ref, other_ref, *outs):
    for chip, out in enumerate(outs):
        out[...] = (
            keep_ref[chip].astype(jnp.float32) + other_ref[chip].astype(jnp.float32)
        ).astype(jnp.bfloat16)


def query_kernel(names, chunk, first, *refs):
    pieces, refs = refs[: len(names)], refs[len(names) :]
    w_refs, gain_ref, refs = refs[: len(names)], refs[len(names)], refs[len(names) + 1 :]
    acc_ref, square_ref = refs[-2:]
    part = pieces[0].shape[1]
    at = places()
    squares = jnp.zeros(square_ref.shape, jnp.float32) if first else refs[1][...]
    for i, name in enumerate(names):
        wide = pieces[i][...].astype(jnp.float32)
        square = wide * wide
        for k in range(part // HEAD_DIM):
            squares += square[:, k * HEAD_DIM : (k + 1) * HEAD_DIM]
        scaled = (wide * gain_ref[at[name], :, chunk * part : (chunk + 1) * part]).astype(jnp.bfloat16)
        w_part = w_refs[i][chunk * part : (chunk + 1) * part, :]
        product = jnp.dot(scaled, w_part, preferred_element_type=jnp.float32)
        if i == 0 and not first:
            acc_ref[...] = refs[0][...] + product
        elif i == 0:
            acc_ref[...] = product
        else:
            acc_ref[...] += product
    square_ref[...] = squares


def dot_nt(left, right):
    return lax.dot_general(left, right, (((1,), (1,)), ((), ())), preferred_element_type=jnp.float32)


def dot_tn(left, right):
    return lax.dot_general(left, right, (((0,), (0,)), ((), ())), preferred_element_type=jnp.float32)


def attention_kernel(
    width,
    acc_ref,
    square_ref,
    own_kv,
    x_kv,
    y_kv,
    d_kv,
    cos_ref,
    sin_ref,
    mask_ref,
    bias_ref,
    kv_bias_ref,
    upstream_ref,
    attended_ref,
    query_grad_ref,
    kv_grad_ref,
    inverse_ref,
):
    rows = acc_ref.shape[0]
    heads = acc_ref.shape[1] // HEAD_DIM
    block = lax.axis_index("tensor")
    scale = HEAD_DIM ** (-0.5)
    inverse = lax.rsqrt(jnp.sum(square_ref[...], axis=1, keepdims=True) / width + EPSILON)
    cosine, sine = cos_ref[...], sin_ref[...]

    def rot(u):
        return u * cosine + pltpu.roll(u, HEAD_DIM // 2, 1) * sine

    def unrot(z):
        return z * cosine - pltpu.roll(z, HEAD_DIM // 2, 1) * sine

    kv_acc = sum(part[...].astype(jnp.float32) for part in (own_kv, x_kv, y_kv, d_kv))
    key_acc, value_acc = kv_acc[:, :HEAD_DIM], kv_acc[:, HEAD_DIM:]
    key = rot(key_acc * inverse + kv_bias_ref[block]).astype(jnp.bfloat16)
    value = (value_acc * inverse + kv_bias_ref[KV_HEADS + block]).astype(jnp.bfloat16)
    parts = [slice(h * HEAD_DIM, (h + 1) * HEAD_DIM) for h in range(heads)]
    bands = [slice(h * rows, (h + 1) * rows) for h in range(heads)]
    accs = [acc_ref[:, part] for part in parts]
    queries = [
        rot(acc * inverse + bias_ref[:, part]).astype(jnp.bfloat16) for acc, part in zip(accs, parts)
    ]
    upstreams = [upstream_ref[:, part] for part in parts]
    all_scores = dot_nt(jnp.concatenate(queries, axis=0), key)
    all_weight_grads = dot_nt(jnp.concatenate(upstreams, axis=0), value)
    scores = [all_scores[band] * scale + mask_ref[...] for band in bands]
    weight_grads = [all_weight_grads[band] for band in bands]
    highest = [jnp.max(score, axis=1, keepdims=True) for score in scores]
    exponents = [jnp.exp(score - high) for score, high in zip(scores, highest)]
    scales = [1.0 / jnp.sum(exponent, axis=1, keepdims=True) for exponent in exponents]
    weights = [exponent * one for exponent, one in zip(exponents, scales)]
    row_inners = [
        jnp.sum(weight * grad, axis=1, keepdims=True) for weight, grad in zip(weights, weight_grads)
    ]
    lows = [weight.astype(jnp.bfloat16) for weight in weights]
    score_grads = [
        (weight * (grad - row_inner)).astype(jnp.bfloat16)
        for weight, grad, row_inner in zip(weights, weight_grads, row_inners)
    ]
    attended = [jnp.dot(low, value, preferred_element_type=jnp.float32) for low in lows]
    turned = [jnp.dot(grad, key, preferred_element_type=jnp.float32) * scale for grad in score_grads]
    inner = jnp.zeros((rows, HEAD_DIM), jnp.float32)
    key_sum = jnp.zeros((HEAD_DIM, rows), jnp.float32)
    value_sum = jnp.zeros((HEAD_DIM, rows), jnp.float32)
    for h, part in enumerate(parts):
        attended_ref[:, part] = attended[h].astype(jnp.bfloat16)
        query_grad = unrot(turned[h]).astype(jnp.bfloat16)
        query_grad_ref[:, part] = query_grad
        inner += query_grad.astype(jnp.float32) * accs[h]
        key_sum += dot_tn(queries[h], score_grads[h])
        value_sum += dot_tn(upstreams[h], lows[h])
    key_grad, value_grad = key_sum.T * scale, value_sum.T
    key_low, value_low = unrot(key_grad).astype(jnp.bfloat16), value_grad.astype(jnp.bfloat16)
    inner += key_low.astype(jnp.float32) * key_acc + value_low.astype(jnp.float32) * value_acc
    kv_grad_ref[:rows, :HEAD_DIM] = key_low
    kv_grad_ref[:rows, HEAD_DIM:] = value_low
    row = lax.broadcasted_iota(jnp.int32, (rows, 2 * HEAD_DIM), 0)
    column = lax.broadcasted_iota(jnp.int32, (rows, 2 * HEAD_DIM), 1)
    column_sum = jnp.sum(inner, axis=1, keepdims=True)
    as_row = jnp.sum(jnp.where(row == column, column_sum, 0.0), axis=0, keepdims=True)
    high = as_row.astype(jnp.bfloat16).astype(jnp.float32)
    middle = (as_row - high).astype(jnp.bfloat16).astype(jnp.float32)
    last = as_row - high - middle
    index = lax.broadcasted_iota(jnp.int32, (EXTRA, 2 * HEAD_DIM), 0)
    tail = jnp.where(index == 0, high, 0.0)
    tail = jnp.where(index == 1, middle, tail)
    tail = jnp.where(index == 2, last, tail)
    kv_grad_ref[rows:, :] = tail.astype(jnp.bfloat16)
    inverse_ref[...] = jnp.broadcast_to(inverse, inverse_ref.shape)


def gradient_kernel(grad_ref, w_ref, *refs):
    added, out_ref = refs[:-1], refs[-1]
    total = dot_nt(grad_ref[...], w_ref[...])
    for more in added:
        total += more[...].astype(jnp.float32)
    out_ref[...] = total.astype(out_ref.dtype)


def add_kernel(left_ref, right_ref, out_ref):
    out_ref[...] = (left_ref[...] + right_ref[...].astype(jnp.float32)).astype(out_ref.dtype)


def keyvalue_gradient_kernel(*refs):
    pieces, (before_ref, w_ref, out_ref, inner_ref, joined) = refs[:-5], refs[-5:]
    rows = out_ref.shape[0]
    half = len(pieces) * HEAD_DIM
    at = places()
    tail = jnp.zeros((EXTRA, 2 * HEAD_DIM), jnp.float32)
    for i, piece in enumerate(pieces):
        for part in range(2):
            start = pl.multiple_of(part * half + at[i] * HEAD_DIM, HEAD_DIM)
            joined[:, pl.ds(start, HEAD_DIM)] = piece[:rows, part * HEAD_DIM : (part + 1) * HEAD_DIM]
        tail += piece[rows:, :].astype(jnp.float32)
    out_ref[...] = before_ref[...] + dot_nt(joined[...], w_ref[...])
    as_row = jnp.sum(tail, axis=0, keepdims=True)
    row = lax.broadcasted_iota(jnp.int32, (rows, 2 * HEAD_DIM), 0)
    column = lax.broadcasted_iota(jnp.int32, (rows, 2 * HEAD_DIM), 1)
    as_column = jnp.sum(jnp.where(row == column, as_row, 0.0), axis=1, keepdims=True)
    inner_ref[...] = jnp.broadcast_to(as_column, inner_ref.shape)


def finish_kernel(width, sum_ref, mate_ref, last_ref, inner_ref, inverse_ref, gain_ref, x_ref, out_ref, band_ref, sems):
    gain = gain_ref[lax.axis_index("tensor")]
    bands, size = band_ref.shape[:2]
    copies = []
    for i in range(bands):
        span = slice(i * size, (i + 1) * size)
        inverse = inverse_ref[span, :1]
        factor = inverse * inverse * inverse * (inner_ref[span, :1] / width)
        normed_grad = sum_ref[span, :] + mate_ref[span, :].astype(jnp.float32)
        normed_grad += last_ref[span, :].astype(jnp.float32)
        band_ref[i] = (
            inverse * (gain * normed_grad) - x_ref[span, :].astype(jnp.float32) * factor
        ).astype(jnp.bfloat16)
        copies.append(pltpu.make_async_copy(band_ref.at[i], out_ref.at[span], sems.at[i]))
        copies[-1].start()
    for copy in copies:
        copy.wait()


def cube_device(
    hidden_slots,
    lengths,
    owners,
    norm_gain,
    w_query,
    query_bias,
    w_keyvalue,
    keyvalue_bias,
    grad_attention,
):
    window, depth = hidden_slots.shape[1:]
    owner_count, lane_count = lax.axis_size("dp"), lax.axis_size("tensor")
    rows, columns = grad_attention.shape
    width, part = depth * lane_count, depth // CHUNKS
    half, full = jnp.bfloat16, jnp.float32

    def permute(value, partner):
        return lax.ppermute(value, "tensor", [(i, partner(i)) for i in range(lane_count)])

    def swap(value):
        return permute(value, lambda i: i ^ 1)

    def near(value):
        return permute(value, lambda i: i ^ (4 if i & 1 else 2))

    def far(value):
        return permute(value, lambda i: i ^ (2 if i & 1 else 4))

    windows = call(
        pick_kernel,
        [((window, part), half)] * (owner_count * CHUNKS),
        [(owners, HBM), (hidden_slots, HBM)],
        scratch=[
            pltpu.SMEM(owners.shape, jnp.int32),
            pltpu.VMEM(hidden_slots.shape, half),
            pltpu.SemaphoreType.DMA((2,)),
        ],
        moved=4 * hidden_slots.size,
    )
    arrived = [[windows[chunk]] for chunk in range(CHUNKS)]
    for chunk in range(CHUNKS):
        for shift in range(1, owner_count):
            pairs = [(i, (i + shift) % owner_count) for i in range(owner_count)]
            arrived[chunk].append(lax.ppermute(windows[shift * CHUNKS + chunk], "dp", pairs))
    frequency = ROPE_BASE ** (-2.0 * jnp.arange(HEAD_DIM // 2, dtype=full) / HEAD_DIM)
    frequency = jnp.concatenate([frequency, frequency])[None]
    w_kv, gain, bias, kv_bias, upstream, chosen, cosine, sine, mask, *w = call(
        functools.partial(prepare_kernel, window),
        [
            (w_keyvalue.shape, half),
            ((lane_count, 1, depth), full),
            ((1, columns), full),
            ((2 * KV_HEADS, 1, HEAD_DIM), full),
            (grad_attention.shape, half),
            ((owner_count, rows, window), half),
            ((rows, HEAD_DIM), full),
            ((rows, HEAD_DIM), full),
            ((rows, rows), full),
        ]
        + [((depth, columns), half)] * lane_count,
        [
            (lengths, HBM),
            (owners, HBM),
            (frequency, VMEM),
            (w_keyvalue, HBM),
            (norm_gain.reshape(lane_count, 1, depth), HBM),
            (query_bias.reshape(1, columns), HBM),
            (keyvalue_bias.reshape(2 * KV_HEADS, 1, HEAD_DIM), HBM),
            (grad_attention, HBM),
            (w_query, HBM),
        ],
        scratch=[
            pltpu.SMEM(lengths.shape, jnp.int32),
            pltpu.SMEM(owners.shape, jnp.int32),
            pltpu.SemaphoreType.DMA((7 + lane_count,)),
        ],
        flops=64 * rows * rows,
        moved=2 * w_query.size,
        need=32,
    )
    sums = None

    def query(chunk, names, pieces):
        nonlocal sums
        sums = call(
            functools.partial(query_kernel, names, chunk, sums is None),
            [((rows, columns), full), ((rows, HEAD_DIM), full)],
            [(piece, VMEM) for piece in pieces]
            + [(w[name], VMEM) for name in names]
            + [(gain, VMEM)]
            + [(value, VMEM) for value in sums or ()],
            flops=2 * rows * part * columns * len(names),
            moved=len(names) * part * columns * 2,
        )

    local, groups = [], []
    for chunk in range(CHUNKS):
        (own,) = call(
            pack_kernel,
            [((rows, part), half)],
            [(chosen, VMEM)] + [(piece, VMEM) for piece in arrived[chunk]],
            flops=2 * rows * window * owner_count * part,
            moved=4 * rows * part * 2,
        )
        local.append(own)
        a0 = near(own)
        mate = swap(own)
        a1 = near(mate)
        b0 = swap(a0)
        c0 = far(a0)
        b1 = swap(a1)
        c1 = swap(c0)
        groups.append([own, mate, a0, a1, b0, b1, c0, c1])
    for chunk in range(CHUNKS):
        group = groups[chunk]
        for names in GROUPS:
            query(chunk, names, [group[n] for n in names])
    acc, square = sums

    kv_shape = (lane_count // 2, rows, 2 * HEAD_DIM)
    keep, send = call(
        keyvalue_kernel,
        [(kv_shape, half), (kv_shape, half)],
        [(piece, VMEM) for piece in local] + [(gain, VMEM), (w_kv, VMEM)],
        scratch=[pltpu.VMEM((lane_count, rows, 2 * HEAD_DIM), half)],
        flops=2 * rows * depth * w_keyvalue.shape[1],
        moved=w_keyvalue.size * 2,
        need=16,
    )
    other = swap(send)
    kv_parts = call(
        chip_sum_kernel,
        [(kv_shape[1:], half)] * (lane_count // 2),
        [(keep, VMEM), (other, VMEM)],
        flops=rows * depth,
        moved=rows * depth * 6,
    )
    kv_parts = [kv_parts[0]] + [
        permute(kv_parts[chip], lambda i, chip=chip: i ^ (2 * chip))
        for chip in range(1, lane_count // 2)
    ]

    attended, query_grad, kv_grad, inverse = call(
        functools.partial(attention_kernel, width),
        [
            ((rows, columns), half),
            ((rows, columns), half),
            ((rows + EXTRA, 2 * HEAD_DIM), half),
            ((rows, HEAD_DIM), full),
        ],
        [(acc, VMEM), (square, VMEM)]
        + [(piece, VMEM) for piece in kv_parts]
        + [(value, VMEM) for value in (cosine, sine, mask, bias, kv_bias, upstream)],
        flops=14 * rows * rows * columns,
        moved=rows * columns * 10,
        need=32,
    )

    def gradient(name, added=(), kind=half):
        return call(
            gradient_kernel,
            [((rows, depth), kind)],
            [(query_grad, VMEM), (w[name], VMEM)] + [(value, VMEM) for value in added],
            flops=2 * rows * depth * columns,
            moved=depth * columns * 2,
        )

    (to_c1,) = gradient(C1)
    from_c1 = swap(to_c1)
    (to_b1,) = gradient(B1)
    from_b1 = swap(to_b1)
    (to_c0,) = gradient(C0, (from_c1,))
    from_far = far(to_c0)
    (to_a1,) = gradient(A1, (from_b1,))
    near_mate = near(to_a1)
    (to_b0,) = gradient(B0)
    from_b0 = swap(to_b0)

    kv_mate, kv_a0 = swap(kv_grad), near(kv_grad)
    kv_a1 = near(kv_mate)
    kv_b0, kv_c0 = swap(kv_a0), far(kv_a0)
    kv_b1, kv_c1 = swap(kv_a1), swap(kv_c0)

    (part_a0,) = gradient(A0, (from_b0,), full)
    (to_a0,) = call(
        add_kernel,
        [((rows, depth), half)],
        [(part_a0, VMEM), (from_far, VMEM)],
        flops=rows * depth,
        moved=rows * depth * 8,
    )
    near_own = near(to_a0)
    (to_own,) = gradient(OWN, (), full)
    (to_mate,) = gradient(MATE, (near_mate,))
    from_mate = swap(to_mate)
    total, inner = call(
        keyvalue_gradient_kernel,
        [((rows, depth), full), ((rows, HEAD_DIM), full)],
        [(piece, VMEM) for piece in (kv_grad, kv_mate, kv_a0, kv_a1, kv_b0, kv_b1, kv_c0, kv_c1)]
        + [(to_own, VMEM), (w_kv, VMEM)],
        scratch=[pltpu.VMEM((rows, w_keyvalue.shape[1]), half)],
        flops=2 * rows * depth * w_keyvalue.shape[1],
        moved=w_keyvalue.size * 2,
        need=16,
    )
    (input_grad,) = call(
        functools.partial(finish_kernel, width),
        [jax.ShapeDtypeStruct((rows, depth), half)],
        [(value, VMEM) for value in (total, from_mate, near_own, inner, inverse, gain, *local)],
        scratch=[
            pltpu.VMEM((BANDS, rows // BANDS, depth), half),
            pltpu.SemaphoreType.DMA((BANDS,)),
        ],
        flops=8 * rows * depth,
        moved=rows * depth * 14,
    )
    return attended, input_grad


def solution(mesh):
    in_specs = (
        P("dp", None, "tensor"),
        P(),
        P(),
        P(),
        P(None, "tensor"),
        P("tensor"),
        P("tensor", None),
        P(),
        P("dp", "tensor"),
    )
    out_specs = (P("dp", "tensor"), P("dp", "tensor"))
    cube = mesh.shape["tensor"] == 8 and KV_HEADS == 8

    def layer(*args):
        return cube_device(*args)

    return jax.shard_map(
        layer if cube else on_device,
        mesh=mesh,
        in_specs=in_specs,
        out_specs=out_specs,
        check_vma=False,
    )
```
